32 devices in a mesh: gx: 2 (over x), gy: 4 (over z), gz: 4 (over y, core).
Axes of the slice: x: 2, y: 2, z: 4, core: 2. Of those that a mesh axis runs over, the one named last changes fastest.
Arguments:
- right_side: float32 [48, 96, 512], P('gx', 'gy', 'gz'), may hold values from -6 to 6
- reaction: float32 [48, 96, 512], P('gx', 'gy', 'gz'), may hold values from 0.05 to 2
- basis_x: float32 [40, 40], replicated, may hold values from -1 to 1
- basis_y: float32 [40, 40], replicated, may hold values from -1 to 1
- basis_z: float32 [144, 144], replicated, may hold values from -0.5 to 0.5
- eigen_x: float32 [40], replicated, may hold values from 0.5 to 6
- eigen_y: float32 [40], replicated, may hold values from 0.5 to 6
- eigen_z: float32 [144], replicated, may hold values from 0.5 to 6
Outputs:
- solution: float32 [48, 96, 512], P('gx', 'gy', 'gz')
The draws below stay inside these ranges and needn't reach their ends.
All inputs are finite; a program needn't handle non-finite values.
Results may differ from the reference program's by a relative error of at most 0.0003.
Values sent between devices are 32-bit elements; how exact they have to be, the bound alone decides.
No kernel may reach another device: no remote copies, remote signals or barrier semaphores. Data moves between devices by JAX's collectives and lax.ppermute only.
A program may use at most 64 MiB of HBM per device.

```python
import math
import jax
import jax.numpy as jnp
from jax import lax

CX = 24
CY = 24
CZ = 128
OV = 8
EX = 40
EY = 40
EZ = 144
NX = 48
NY = 96
NZ = 512
N_GX = 2
N_GY = 4
N_GZ = 4


def block_scale(stream_key, shape, pieces, low, high):
    def one(dim, blocks):
        heights = jax.random.uniform(jax.random.fold_in(jax.random.fold_in(stream_key, 6), dim), (blocks,), jnp.float32, low / len(pieces), high / len(pieces))
        return jnp.repeat(jnp.exp(heights), shape[dim] // blocks).reshape((-1,) + (1,) * (len(shape) - dim - 1))

    factor_of = one(*pieces[0])
    for cut in pieces[1:]:
        factor_of = factor_of * one(*cut)
    return factor_of


def normal_values(key, shape, scale, reach, cuts=(), kind=jnp.bfloat16):
    drawn = scale * jax.random.normal(key, shape, jnp.float32)
    if cuts:
        drawn = drawn * block_scale(key, shape, cuts, -0.22, 0.18)
    return jnp.clip(drawn, -reach, reach).astype(kind)


def setup_inputs(seed: int = 0) -> dict:
    keys = jax.random.split(jax.random.key(seed), 9)
    return {
        "right_side": normal_values(keys[0], (NX, NY, NZ), 1.0, 6.0, ((0, 2), (1, 4), (2, 4)), jnp.float32),
        "reaction": jnp.clip(jnp.exp(math.log(2.0) - 3.6888794 * jax.random.uniform(keys[1], (NX, NY, NZ), jnp.float32) ** block_scale(keys[1], (NX, NY, NZ), ((0, 2), (1, 4), (2, 4)), -0.2, 0.2)), 0.05, 2.0),
        "basis_x": normal_values(keys[2], (EX, EX), EX ** -0.5, 1.0, (), jnp.float32),
        "basis_y": normal_values(keys[3], (EY, EY), EY ** -0.5, 1.0, (), jnp.float32),
        "basis_z": normal_values(keys[4], (EZ, EZ), EZ ** -0.5, 0.5, (), jnp.float32),
        "eigen_x": jnp.clip(jnp.exp(jax.random.uniform(keys[5], (EX,), jnp.float32, math.log(0.5), math.log(6.0))), 0.5, 6.0),
        "eigen_y": jnp.clip(jnp.exp(jax.random.uniform(keys[6], (EY,), jnp.float32, math.log(0.5), math.log(6.0))), 0.5, 6.0),
        "eigen_z": jnp.clip(jnp.exp(jax.random.uniform(keys[7], (EZ,), jnp.float32, math.log(0.5), math.log(6.0))), 0.5, 6.0),
    }


def stencil(padded, coefficient):
    center = padded[1:-1, 1:-1, 1:-1]
    sizes = center.shape
    total = coefficient * center
    weights = {1: 0.5, 2: 0.125, 3: 0.0625}
    for offset_x in (-1, 0, 1):
        for offset_y in (-1, 0, 1):
            for offset_z in (-1, 0, 1):
                count = abs(offset_x) + abs(offset_y) + abs(offset_z)
                if count == 0:
                    continue
                neighbour = padded[1 + offset_x:1 + offset_x + sizes[0], 1 + offset_y:1 + offset_y + sizes[1], 1 + offset_z:1 + offset_z + sizes[2]]
                total = total + weights[count] * (center - neighbour)
    return total


def local_solve(block, basis_x, basis_y, basis_z, eigen_x, eigen_y, eigen_z):
    highest = lax.Precision.HIGHEST
    modes = jnp.einsum('ap,abc->pbc', basis_x, block, precision=highest)
    modes = jnp.einsum('bq,pbc->pqc', basis_y, modes, precision=highest)
    modes = jnp.einsum('cs,pqc->pqs', basis_z, modes, precision=highest)
    modes = modes / (eigen_x[:, None, None] + eigen_y[None, :, None] + eigen_z[None, None, :])
    back = jnp.einsum('ap,pqs->aqs', basis_x, modes, precision=highest)
    back = jnp.einsum('bq,aqs->abs', basis_y, back, precision=highest)
    back = jnp.einsum('cs,abs->abc', basis_z, back, precision=highest)
    return back


def reference(right_side, reaction, basis_x, basis_y, basis_z, eigen_x, eigen_y, eigen_z):
    extent = (CX + 2 * OV, CY + 2 * OV, CZ + 2 * OV)

    def schwarz(field):
        padded = jnp.pad(field, OV)
        empty = jnp.zeros(padded.shape, jnp.float32)

        def visit(total, index):
            first_index = index // (N_GY * N_GZ)
            second_index = (index // N_GZ) % N_GY
            third_index = index % N_GZ
            starts = ((first_index * CX).astype(jnp.int32), (second_index * CY).astype(jnp.int32), (third_index * CZ).astype(jnp.int32))
            block = lax.dynamic_slice(padded, starts, extent)
            correction = local_solve(block, basis_x, basis_y, basis_z, eigen_x, eigen_y, eigen_z)
            updated = lax.dynamic_slice(total, starts, extent) + correction
            return lax.dynamic_update_slice(total, updated, starts), None

        total, unused = lax.scan(visit, empty, jnp.arange(N_GX * N_GY * N_GZ, dtype=jnp.int32))
        return total[OV:-OV, OV:-OV, OV:-OV]

    first = schwarz(right_side)
    residual = right_side - stencil(jnp.pad(first, 1), reaction)
    solution = first + schwarz(residual)
    return solution
```

```python
import jax
import jax.numpy as jnp
from jax import lax
from jax.sharding import PartitionSpec as P


def pairs(count, first):
    swaps = {}
    for low in range(first, count - 1, 2):
        swaps[low], swaps[low + 1] = low + 1, low
    return [(i, swaps.get(i, i)) for i in range(count)]


def swap_slabs(low, high, axis):
    count = lax.axis_size(axis)
    index = lax.axis_index(axis)
    even = index % 2 == 0
    one = lax.ppermute(jnp.where(even, high, low), axis, pairs(count, 0))
    two = lax.ppermute(jnp.where(even, low, high), axis, pairs(count, 1))
    below = jnp.where(index > 0, jnp.where(even, two, one), 0.0)
    above = jnp.where(index < count - 1, jnp.where(even, one, two), 0.0)
    return below, above


def gather_x(block):
    count = lax.axis_size("gx")
    parts = [block]
    for shift in range(1, count):
        parts.append(lax.ppermute(block, "gx", [((i + shift) % count, i) for i in range(count)]))
    return jnp.concatenate(parts, axis=1)


def widen(core, width):
    low, high = swap_slabs(core[:width], core[-width:], "gy")
    core = jnp.concatenate([low, core, high], axis=0)
    rows = core.shape[0] * core.shape[1]
    flat = core.reshape(rows, core.shape[2])
    low, high = swap_slabs(flat[:, :width].T, flat[:, -width:].T, "gz")
    flat = jnp.concatenate([low.T, flat, high.T], axis=1)
    return flat.reshape(core.shape[0], core.shape[1], -1)


def spread(piece, before, after, dim):
    pad = [(0, 0)] * piece.ndim
    pad[dim] = (before, after)
    return jnp.pad(piece, pad)


def local(right_side, reaction, basis_x, basis_y, basis_z, eigen_x, eigen_y, eigen_z):
    cx, cy, cz = right_side.shape
    ex, ey, ez = basis_x.shape[0], basis_y.shape[0], basis_z.shape[0]
    ov = (ex - cx) // 2
    nx, ny, nz = lax.axis_size("gx"), lax.axis_size("gy"), lax.axis_size("gz")
    ix, iy, iz = lax.axis_index("gx"), lax.axis_index("gy"), lax.axis_index("gz")
    all_x = nx * cx
    high = lax.Precision.HIGH

    blocks = [spread(basis_x.T, i * cx, (nx - 1 - i) * cx, 1)[:, ov : ov + all_x] for i in range(nx)]
    table = jnp.concatenate(blocks, axis=0)
    turned = lax.dynamic_slice_in_dim(jnp.concatenate([table, table], axis=1), ix * cx, all_x, axis=1)
    eigen = jnp.tile(eigen_x, nx)[None, :, None] + eigen_y[:, None, None] + eigen_z[None, None, :]

    def solve(block, back_rows):
        modes = jnp.einsum("zs,yxz->yxs", basis_z, block, precision=high)
        modes = jnp.einsum("rx,yxs->yrs", turned, modes, precision=high)
        modes = jnp.einsum("yq,yrs->qrs", basis_y, modes, precision=high)
        modes = modes / eigen
        back = jnp.einsum("yq,qrs->yrs", basis_y, modes, precision=high)
        back = jnp.einsum("rx,yrs->yxs", turned[:, :back_rows], back, precision=high)
        return jnp.einsum("zs,yxs->yxz", basis_z, back, precision=high)

    f = gather_x(right_side.transpose(1, 0, 2))
    c = gather_x(reaction.transpose(1, 0, 2))
    f = widen(f, ov)
    c = widen(c, ov)

    u = solve(f, all_x)
    w = 2 * ov + 1
    core, side = u[:, :, ov : ov + cz], jnp.concatenate([u[:, :, :ov], u[:, :, ov + cz :]], axis=2)
    low, up = swap_slabs(core[:w], core[-w:], "gy")
    core = spread(core, 1, 1, 0) + spread(low, 0, cy + 1, 0) + spread(up, cy + 1, 0, 0)
    side_low, side_up = swap_slabs(side[:w].reshape(w * all_x, -1).T, side[-w:].reshape(w * all_x, -1).T, "gy")
    side_low, side_up = side_low.T.reshape(w, all_x, -1), side_up.T.reshape(w, all_x, -1)
    side = spread(side, 1, 1, 0) + spread(side_low, 0, cy + 1, 0) + spread(side_up, cy + 1, 0, 0)
    v = jnp.concatenate([side[:, :, :ov], core, side[:, :, ov:]], axis=2)
    rows = v.shape[0] * all_x
    flat = v.reshape(rows, ez)
    low, up = swap_slabs(flat[:, :w].T, flat[:, -w:].T, "gz")
    flat = spread(flat, 1, 1, 1) + spread(low.T, 0, cz + 1, 1) + spread(up.T, cz + 1, 0, 1)
    v = flat.reshape(ey + 2, all_x, ez + 2)
    in_y = (jnp.arange(ey + 2) + iy * cy - ov - 1 >= 0) & (jnp.arange(ey + 2) + iy * cy - ov - 1 < ny * cy)
    in_z = (jnp.arange(ez + 2) + iz * cz - ov - 1 >= 0) & (jnp.arange(ez + 2) + iz * cz - ov - 1 < nz * cz)
    v = jnp.where(in_y[:, None, None] & in_z[None, None, :], v, 0.0)

    sum_y = v[:-2, :, :] + v[2:, :, :]
    v0 = v[1:-1]
    center = v0[:, :, 1:-1]
    p = sum_y[:, :, 1:-1] + v0[:, :, :-2] + v0[:, :, 2:]
    q = sum_y[:, :, :-2] + sum_y[:, :, 2:]
    flat_part = 0.5 * p + 0.125 * q
    side_part = 0.5 * center + 0.125 * p + 0.0625 * q
    x = (jnp.arange(all_x) + ix * cx) % all_x
    from_low = jnp.where((x > 0)[None, :, None], jnp.roll(side_part, 1, axis=1), 0.0)
    from_up = jnp.where((x < all_x - 1)[None, :, None], jnp.roll(side_part, -1, axis=1), 0.0)
    residual = f - ((c + 5.0) * center - flat_part - from_low - from_up)
    residual = jnp.where(in_y[1:-1, None, None] & in_z[None, None, 1:-1], residual, 0.0)

    u = solve(residual, cx)
    flat = u.reshape(ey * cx, ez)
    low, up = swap_slabs(flat[:, :ov].T, flat[:, -ov:].T, "gz")
    core = flat[:, ov : ov + cz] + spread(low.T, 0, cz - ov, 1) + spread(up.T, cz - ov, 0, 1)
    core = core.reshape(ey, cx, cz)
    low, up = swap_slabs(core[:ov], core[-ov:], "gy")
    own = core[ov : ov + cy] + spread(low, 0, cy - ov, 0) + spread(up, cy - ov, 0, 0)
    total = own + v[ov + 1 : ov + 1 + cy, :cx, ov + 1 : ov + 1 + cz]
    return total.transpose(1, 0, 2)


def solution(mesh):
    return jax.shard_map(
        local,
        mesh=mesh,
        in_specs=(P("gx", "gy", "gz"), P("gx", "gy", "gz"), P(), P(), P(), P(), P(), P()),
        out_specs=P("gx", "gy", "gz"),
        check_vma=False,
    )
```

```python
import functools
import math

import jax
import jax.numpy as jnp
from jax import lax
from jax.experimental import pallas as pl
from jax.experimental.pallas import tpu as pltpu
from jax.sharding import PartitionSpec as P

LANES = 128
RING = 256
F32 = jnp.float32
BF16 = jnp.bfloat16


def pairs(count, first):
    swaps = {}
    for low in range(first, count - 1, 2):
        swaps[low], swaps[low + 1] = low + 1, low
    return [(i, swaps.get(i, i)) for i in range(count)]


def swap(one, two, axis):
    count = lax.axis_size(axis)
    return lax.ppermute(one, axis, pairs(count, 0)), lax.ppermute(two, axis, pairs(count, 1))


def call(kernel, outs, *args, scratch=(), smem=1, after=()):
    vmem = pl.BlockSpec(memory_space=pltpu.VMEM)
    specs = [pl.BlockSpec(memory_space=pltpu.SMEM)] * smem + [vmem] * (len(args) - smem)
    specs += [pl.BlockSpec(memory_space=pl.ANY)] * len(after)
    used = len(args)
    held = sum(math.prod(s.shape) * 4 for s in scratch)

    def body(*refs):
        kernel(*refs[:used], *refs[used + len(after) :])

    return pl.pallas_call(
        body,
        out_shape=[jax.ShapeDtypeStruct(s, F32) for s in outs],
        in_specs=specs,
        out_specs=[vmem] * len(outs),
        scratch_shapes=list(scratch),
        compiler_params=pltpu.CompilerParams(vmem_limit_bytes=held + 6 * 1024 * 1024),
    )(*args, *after)


class Side:
    def __init__(self, index, count):
        self.even = index % 2 == 0
        self.has_below = index > 0
        self.has_above = index < count - 1
        self.one_valid = jnp.where(self.even, self.has_above, self.has_below)
        self.two_valid = jnp.where(self.even, self.has_below, self.has_above)

    def one(self, above, below):
        return jnp.where(self.even, above, below)

    def two(self, above, below):
        return jnp.where(self.even, below, above)


def rows_of(start, size):
    return pl.ds(pl.multiple_of(start, 8), size)


def lane_of(shape):
    return lax.broadcasted_iota(jnp.int32, shape, 1)


def group_of(count, width):
    return -(-count // (LANES // width))


def pack(load, count, rows, width, src, out):
    each = group_of(count, width)
    lane = lane_of((rows, LANES))

    def member(j, carry):
        value = jnp.zeros((rows, LANES), F32)
        for g in range(-(-count // each)):
            x = jnp.minimum(g * each + j, count - 1)
            turned = pltpu.roll(load(x), (g * width - src + LANES) % LANES, 1)
            value = jnp.where((lane >= g * width) & (lane < (g + 1) * width), turned, value)
        out[rows_of(j * rows, rows), :] = value
        return carry

    lax.fori_loop(0, each, member, 0, unroll=each <= 3)


def unpack(ref, x, count, rows, width, dst, valid):
    each = group_of(count, width)
    g, j = x // each, x % each
    turned = pltpu.roll(ref[rows_of(j * rows, rows), :], (dst - g * width + LANES) % LANES, 1)
    away = (lane_of((rows, LANES)) - dst + LANES) % LANES
    return jnp.where((away < width) & valid, turned, 0.0)


def split(value):
    high = value.astype(BF16)
    return high, (value - high.astype(F32)).astype(BF16)


def stack_rows(value):
    high, low = split(value)
    return jnp.concatenate([high, high, low], axis=0)


def dot(a, b):
    return jnp.dot(a, b, preferred_element_type=F32)


def dot_nt(a, b):
    return lax.dot_general(a, b, (((1,), (1,)), ((), ())), preferred_element_type=F32)


def first_slabs(info, *refs, ny, ov):
    parts, (one, two) = refs[:-2], refs[-2:]
    side = Side(info[1], ny)
    cx, cy, _ = parts[0].shape
    for k, part in enumerate(parts):
        one[k * cx : (k + 1) * cx] = part[:, rows_of(side.one(cy - ov, 0), ov), :]
        two[k * cx : (k + 1) * cx] = part[:, rows_of(side.two(cy - ov, 0), ov), :]


def second_slabs(info, *refs, ny, nz, ov):
    parts, (got_one, got_two, field, one, two) = refs[:-5], refs[-5:]
    side, along = Side(info[1], ny), Side(info[2], nz)
    cx, cy, cz = parts[0].shape
    ey = cy + 2 * ov
    count = len(parts) * cx
    for k, part in enumerate(parts):

        def place(x, carry, k=k, part=part):
            a = got_one[k * cx + x]
            b = got_two[k * cx + x]
            row = (k * cx + x) * ey
            above = jnp.where(side.even, a, b)
            below = jnp.where(side.even, b, a)
            field[rows_of(row, ov), :] = jnp.where(side.has_below, below, 0.0)
            field[rows_of(row + ov, cy), :] = part[x]
            field[rows_of(row + ov + cy, ov), :] = jnp.where(side.has_above, above, 0.0)
            return carry

        lax.fori_loop(0, cx, place, 0)

    def load(x):
        return field[rows_of(x * ey, ey), :]

    pack(load, count, ey, ov, along.one(cz - ov, 0), one)
    pack(load, count, ey, ov, along.two(cz - ov, 0), two)


def extended(field, got_one, got_two, x, count, ey, ov, along):
    halo = unpack(got_one, x, count, ey, ov, along.one(0, LANES - ov), along.one_valid)
    halo = halo + unpack(got_two, x, count, ey, ov, along.two(0, LANES - ov), along.two_valid)
    return jnp.concatenate([field[rows_of(x * ey, ey), :], halo], axis=1)


def turn(value):
    group = LANES // 8
    row = lax.broadcasted_iota(jnp.int32, (8, LANES), 0)
    column = lane_of((8, LANES)) // group
    for bit in (4, 2, 1):
        up = pltpu.roll(pltpu.roll(value, 8 - bit, 0), bit * group, 1)
        down = pltpu.roll(pltpu.roll(value, bit, 0), LANES - bit * group, 1)
        moved = jnp.where((row & bit) == 0, up, down)
        value = jnp.where((row & bit) == (column & bit), value, moved)
    return value


def solve(source, store, tables, state, count, back, ey):
    zt, y_on, y_back, x_on, x_back, recip = tables
    s0, s1 = state
    z_high, z_low = split(zt[...])
    modes = recip.shape[1]
    group = LANES // 8
    lane = lane_of((ey, LANES))
    octs = ey // 8
    nothing = jnp.zeros((ey, LANES), F32)

    def times_y(table, core, side):
        two = 2 * ey
        first = dot(table[...], stack_rows(jnp.concatenate([core[:two], core[two : 2 * two]], axis=1)))
        second = dot(table[...], stack_rows(jnp.concatenate([core[2 * two : 3 * two], core[3 * two :]], axis=1)))
        third = dot(table[...], stack_rows(jnp.concatenate([side, nothing], axis=0)))
        return jnp.concatenate([first[:, :LANES], first[:, LANES:], second[:, :LANES], second[:, LANES:]], axis=0), third[:ey]

    def on(k, carry):
        high, low = split(jnp.concatenate([source(8 * k + j) for j in range(8)], axis=0))
        value = dot(high, z_high) + (dot(high, z_low) + dot(low, z_high))
        side = nothing
        for j in range(8):
            turned = pltpu.roll(value[j * ey : (j + 1) * ey, LANES:], j * group, 1)
            side = jnp.where(lane // group == j, turned, side)
        core, side = times_y(y_on, value[:, :LANES], side)
        s0[rows_of(k * 8 * ey, 8 * ey), :] = core
        for q in range(octs):
            s1[rows_of(q * count + k * 8, 8), :] = turn(side[q * 8 : (q + 1) * 8])
        return carry

    lax.fori_loop(0, count // 8, on, 0, unroll=2)

    def times_x(value, factor):
        value = dot(x_on[...], stack_rows(value))
        value = jnp.concatenate([value[i * modes : (i + 1) * modes] * factor for i in range(value.shape[0] // modes)], axis=0)
        return dot(x_back[...], stack_rows(value))[:back]

    def middle(h, carry):
        q = 2 * h
        value = [s0[pl.ds(q + i, count, stride=ey), :] for i in range(2)]
        value = times_x(jnp.concatenate(value, axis=1), jnp.concatenate([recip[q], recip[q + 1]], axis=1))
        for i in range(2):
            s0[pl.ds(q + i, back, stride=ey), :] = value[:, i * LANES : (i + 1) * LANES]
        return carry

    for q in range(octs):
        value = times_x(s1[q * count : (q + 1) * count, :], recip[ey + q])
        s1[q * count : q * count + back, :] = value
    lax.fori_loop(0, ey // 2, middle, 0, unroll=4)

    def off(k, carry):
        side = jnp.concatenate([turn(s1[rows_of(q * count + k * 8, 8), :]) for q in range(octs)], axis=0)
        core, side = times_y(y_back, s0[rows_of(k * 8 * ey, 8 * ey), :], side)
        side = jnp.concatenate([side] + [pltpu.roll(side, LANES - j * group, 1) for j in range(1, 8)], axis=0)
        high, low = split(jnp.concatenate([core, side], axis=1))
        value = dot_nt(high, z_high) + (dot_nt(high, z_low) + dot_nt(low, z_high))
        for j in range(8):
            store(8 * k + j, value[j * ey : (j + 1) * ey])
        return carry

    lax.fori_loop(0, back // 8, off, 0, unroll=2 if back % 16 == 0 else 1)


def merged(core, halo, low):
    lane = lane_of(core.shape)
    return jnp.where((lane < LANES // 2) == low, core, halo)


def first_solve(info, field, got_one, got_two, zt, y_on, y_back, x_on, x_back, recip, u, block, one, two, s0, s1, *, nz, ov, ey, cz):
    along = Side(info[2], nz)
    count = field.shape[0] // ey
    w = 2 * ov + 1

    def source(x):
        value = extended(field, got_one, got_two, x, count, ey, ov, along)
        block[rows_of(x * ey, ey), :] = value
        return value

    def store(x, value):
        u[rows_of(x * ey, ey), :] = value

    solve(source, store, (zt, y_on, y_back, x_on, x_back, recip), (s0, s1), count, count, ey)

    for out, low in ((one, ~along.even), (two, along.even)):

        def load(x, low=low):
            rows = rows_of(x * ey, ey)
            return merged(u[rows, :LANES], u[rows, LANES:], low)

        pack(load, count, ey, w, jnp.where(low, LANES - ov, cz - ov - 1), out)


def sum_z(info, u, got_one, got_two, v, one, two, *, ny, nz, ov, ey, cz):
    side, along = Side(info[1], ny), Side(info[2], nz)
    count = u.shape[0] // ey
    w = 2 * ov + 1
    lane = lane_of((ey, LANES))
    inside = ((lane <= ov) & along.has_above) | ((lane >= LANES - ov - 1) & along.has_below)

    def add(x, carry):
        rows = rows_of(x * ey, ey)
        core, rest = u[rows, :LANES], u[rows, LANES:]
        for got, low, valid in ((got_one, ~along.even, along.one_valid), (got_two, along.even, along.two_valid)):
            part = unpack(got, x, count, ey, w, jnp.where(low, LANES - ov - 1, cz - ov), valid)
            mine = (lane < LANES // 2) == low
            core, rest = core + jnp.where(mine, part, 0.0), rest + jnp.where(mine, 0.0, part)
        v[rows, :LANES] = core
        v[rows, LANES:] = jnp.where(inside, rest, 0.0)
        return carry

    lax.fori_loop(0, count, add, 0, unroll=4)
    tall, halo = 2 * ov, 2 * (ov + 1)
    each = group_of(count, halo)
    for out, start, odd in (
        (one, side.one(ey - tall, 0), side.even),
        (two, side.two(ey - tall, 0), ~side.even),
    ):

        def main(x, carry, out=out, start=start):
            out[rows_of(x * tall, tall), :] = v[rows_of(x * ey + start, tall), :LANES]
            return carry

        lax.fori_loop(0, count, main, 0)
        base = count * tall

        def load(x, start=start):
            return v[rows_of(x * ey + start, tall), LANES:]

        pack(load, count, tall, halo, LANES - ov - 1, out.at[base : base + each * tall])
        base = base + each * tall
        for x in range(count):
            last, next_ = v[x * ey + ey - tall - 1 : x * ey + ey - tall, :], v[x * ey + tall : x * ey + tall + 1, :]
            row = jnp.where(odd, last, next_)
            out[base + x : base + x + 1, :] = row[:, :LANES]
            out[base + count + x : base + count + x + 1, :] = row[:, LANES:]


def second_solve(info, v, got_one, got_two, block, coef, c_one, c_two, zt, y_on, y_back, x_on, x_back, recip, u, first, one, two, s0, s1, side_part, resid, *, nx, ny, nz, ov, ey, cx, cz):
    side, along = Side(info[1], ny), Side(info[2], nz)
    count = coef.shape[0] // ey
    tall, halo = 2 * ov, 2 * (ov + 1)
    each = group_of(count, halo)
    cy = ey - 2 * ov
    main_rows = count * tall
    odd_rows = main_rows + each * tall

    def slab(ref, x, valid):
        core = ref[rows_of(x * tall, tall), :]
        extra = unpack(ref.at[main_rows:odd_rows], x, count, tall, halo, LANES - ov - 1, True)
        return jnp.where(valid, jnp.concatenate([core, extra], axis=1), 0.0)

    def odd(ref, x, valid):
        row = jnp.concatenate([ref[pl.ds(odd_rows + x, 1), :], ref[pl.ds(odd_rows + count + x, 1), :]], axis=1)
        return jnp.where(valid, row, 0.0)

    def gather(x, carry):
        a, b = slab(got_one, x, side.one_valid), slab(got_two, x, side.two_valid)
        above, below = jnp.where(side.even, a, b), jnp.where(side.even, b, a)
        value = v[rows_of(x * ey, ey), :]
        value = jnp.concatenate([value[:tall] + below, value[tall : ey - tall], value[ey - tall :] + above], axis=0)
        y = lax.broadcasted_iota(jnp.int32, (ey, RING), 0)
        value = jnp.where(((y >= ov) | side.has_below) & ((y < ey - ov) | side.has_above), value, 0.0)
        a, b = odd(got_one, x, side.one_valid), odd(got_two, x, side.two_valid)
        near = lax.broadcasted_iota(jnp.int32, (8, RING), 0)
        under = jnp.where(near == 7, jnp.where(side.even, b, a), 0.0)
        over = jnp.where(near == 0, jnp.where(side.even, a, b), 0.0)
        center = value
        full = jnp.concatenate([under, value, over], axis=0)
        sum_y = full[7 : 7 + ey] + full[9 : 9 + ey]

        @pl.when(x < cx)
        def _():
            first[rows_of(x * cy, cy), :] = center[ov : ov + cy, :LANES]

        p = sum_y + pltpu.roll(center, 1, 1) + pltpu.roll(center, RING - 1, 1)
        q = pltpu.roll(sum_y, 1, 1) + pltpu.roll(sum_y, RING - 1, 1)
        f = block[rows_of(x * ey, ey), :]
        c = extended(coef, c_one, c_two, x, count, ey, ov, along)
        rows = rows_of(x * ey, ey)
        side_part[rows, :] = 0.5 * center + 0.125 * p + 0.0625 * q
        resid[rows, :] = f - (c + 5.0) * center + (0.5 * p + 0.125 * q)
        return carry

    lax.fori_loop(0, count, gather, 0, unroll=2)

    lane = lane_of((ey, RING))
    y = lax.broadcasted_iota(jnp.int32, (ey, RING), 0)
    inside = (lane < cz) | ((lane < cz + ov) & along.has_above) | ((lane >= RING - ov) & along.has_below)
    inside = inside & ((y >= ov) | side.has_below) & ((y < ey - ov) | side.has_above)

    def plane(x):
        at = (info[0] * cx + x) % count
        value = resid[rows_of(x * ey, ey), :]
        before = side_part[rows_of((x + count - 1) % count * ey, ey), :]
        after = side_part[rows_of((x + 1) % count * ey, ey), :]
        value = value + jnp.where(at > 0, before, 0.0) + jnp.where(at < count - 1, after, 0.0)
        return jnp.where(inside, value, 0.0)

    def store(x, value):
        rows = rows_of(x * ey, ey)
        u[rows, :] = value[:, :LANES]
        resid[rows, :LANES] = value[:, LANES:]

    solve(plane, store, (zt, y_on, y_back, x_on, x_back, recip), (s0, s1), count, cx, ey)

    def load(x):
        return resid[rows_of(x * ey, ey), :LANES]

    pack(load, cx, ey, ov, along.one(0, LANES - ov), one)
    pack(load, cx, ey, ov, along.two(0, LANES - ov), two)


def last_sum_z(info, u, got_one, got_two, v, one, two, *, ny, nz, ov, ey, cx, cz):
    side, along = Side(info[1], ny), Side(info[2], nz)

    def add(x, carry):
        rows = rows_of(x * ey, ey)
        value = u[rows, :]
        value = value + unpack(got_one, x, cx, ey, ov, along.one(cz - ov, 0), along.one_valid)
        value = value + unpack(got_two, x, cx, ey, ov, along.two(cz - ov, 0), along.two_valid)
        v[rows, :] = value
        one[rows_of(x * ov, ov), :] = v[rows_of(x * ey + side.one(ey - ov, 0), ov), :]
        two[rows_of(x * ov, ov), :] = v[rows_of(x * ey + side.two(ey - ov, 0), ov), :]
        return carry

    lax.fori_loop(0, cx, add, 0)


def last_sum_y(info, v, got_one, got_two, first, out, *, ny, ov, ey, cx):
    side = Side(info[1], ny)
    cy = ey - 2 * ov

    def add(x, carry):
        a, b = got_one[rows_of(x * ov, ov), :], got_two[rows_of(x * ov, ov), :]
        above, below = jnp.where(side.even, a, b), jnp.where(side.even, b, a)
        above, below = jnp.where(side.has_above, above, 0.0), jnp.where(side.has_below, below, 0.0)
        value = v[rows_of(x * ey + ov, cy), :] + first[rows_of(x * cy, cy), :]
        out[x] = jnp.concatenate([value[:ov] + below, value[ov : cy - ov], value[cy - ov :] + above], axis=0)
        return carry

    lax.fori_loop(0, cx, add, 0)


def reciprocals(eigen_x, rest, out):
    def row(q, carry):
        out[q] = 1.0 / (eigen_x[...] + rest[pl.ds(q, 1), :])
        return carry

    lax.fori_loop(0, out.shape[0], row, 0, unroll=5)


def gather_x(block):
    count = lax.axis_size("gx")
    return [block] + [lax.ppermute(block, "gx", [((i + shift) % count, i) for i in range(count)]) for shift in range(1, count)]


def columns(table):
    high = lax.reduce_precision(table, 8, 7)
    return jnp.concatenate([high, table - high, high], axis=1).astype(BF16)


def local(right_side, reaction, basis_x, basis_y, basis_z, eigen_x, eigen_y, eigen_z):
    cx, cy, cz = right_side.shape
    ex, ey, ez = basis_x.shape[0], basis_y.shape[0], basis_z.shape[0]
    ov = (ex - cx) // 2
    nx, ny, nz = lax.axis_size("gx"), lax.axis_size("gy"), lax.axis_size("gz")
    ix, iy, iz = lax.axis_index("gx"), lax.axis_index("gy"), lax.axis_index("gz")
    count = nx * cx
    info = jnp.stack([ix, iy, iz]).astype(jnp.int32)
    w, tall, halo = 2 * ov + 1, 2 * ov, 2 * (ov + 1)
    at = dict(ov=ov, ey=ey, cz=cz)

    f_parts = gather_x(right_side)
    c_parts = gather_x(lax.optimization_barrier((reaction, f_parts[-1]))[0])

    blocks = [jnp.pad(basis_x.T, ((0, 0), (i * cx, (nx - 1 - i) * cx)))[:, ov : ov + count] for i in range(nx)]
    table = jnp.concatenate(blocks, axis=0)
    table = lax.dynamic_slice_in_dim(jnp.concatenate([table, table], axis=1), ix * cx, count, axis=1)
    zero = jnp.zeros((ey, ey), F32)
    double = jnp.concatenate([jnp.concatenate([basis_y, zero], axis=1), jnp.concatenate([zero, basis_y], axis=1)], axis=0)
    zt = jnp.concatenate([basis_z[ov:], jnp.zeros((RING - ez, ez), F32), basis_z[:ov]], axis=0)
    zt = jnp.pad(zt, ((0, 0), (0, RING - ez)))
    rest = eigen_y[:, None] + eigen_z[None, :]
    rest = jnp.concatenate([rest[:, :LANES], rest[:, LANES:].reshape(-1, LANES)], axis=0)
    recip = call(reciprocals, [(rest.shape[0], ex, LANES)], jnp.broadcast_to(eigen_x[:, None], (ex, LANES)), rest, smem=0)[0]
    tables = (zt, columns(double.T), columns(double), columns(table), columns(table.T), recip)

    def y_slabs(parts, after=()):
        return call(functools.partial(first_slabs, ny=ny, ov=ov), [(count, ov, cz)] * 2, info, *parts, after=after)

    def z_slabs(parts, got, after=()):
        small = (group_of(count, ov) * ey, LANES)
        return call(functools.partial(second_slabs, ny=ny, nz=nz, ov=ov), [(count * ey, cz), small, small], info, *parts, *got, after=after)

    f, *slabs = z_slabs(f_parts, swap(*y_slabs(f_parts), "gy"))
    c_slabs = y_slabs(c_parts, after=slabs[:1])
    got, c_got = swap(*slabs, "gz"), swap(*c_slabs, "gy")
    state = [pltpu.VMEM((count * ey, LANES), F32), pltpu.VMEM((ey // 8 * count, LANES), F32)]
    small = (group_of(count, w) * ey, LANES)
    u, block, *slabs = call(
        functools.partial(first_solve, nz=nz, **at), [(count * ey, RING)] * 2 + [small, small], info, f, *got, *tables, scratch=state, after=c_slabs[:1]
    )
    c, *c_slabs = z_slabs(c_parts, c_got, after=slabs[:1])
    got, c_got = swap(*slabs, "gz"), swap(*c_slabs, "gz")
    tall_rows = (count * tall + group_of(count, halo) * tall + 2 * count, LANES)
    v, *slabs = call(functools.partial(sum_z, ny=ny, nz=nz, **at), [(count * ey, RING), tall_rows, tall_rows], info, u, *got, after=c_slabs[:1])
    got = swap(*slabs, "gy")
    small = (group_of(cx, ov) * ey, LANES)
    state = state + [pltpu.VMEM((count * ey, RING), F32)] * 2
    u, first, *slabs = call(
        functools.partial(second_solve, nx=nx, ny=ny, nz=nz, cx=cx, **at),
        [(cx * ey, LANES), (cx * cy, LANES), small, small], info, v, *got, block, c, *c_got, *tables, scratch=state,
    )
    got = swap(*slabs, "gz")
    v, *slabs = call(functools.partial(last_sum_z, ny=ny, nz=nz, cx=cx, **at), [(cx * ey, LANES)] + [(cx * ov, LANES)] * 2, info, u, *got)
    got = swap(*slabs, "gy")
    return call(functools.partial(last_sum_y, ny=ny, ov=ov, ey=ey, cx=cx), [(cx, cy, cz)], info, v, *got, first)[0]


def solution(mesh):
    return jax.shard_map(
        local,
        mesh=mesh,
        in_specs=(P("gx", "gy", "gz"), P("gx", "gy", "gz"), P(), P(), P(), P(), P(), P()),
        out_specs=P("gx", "gy", "gz"),
        check_vma=False,
    )
```

```python
import functools
import math

import jax
import jax.numpy as jnp
from jax import lax
from jax.experimental import pallas as pl
from jax.experimental.pallas import tpu as pltpu
from jax.sharding import PartitionSpec as P


LANES = 128
RING = 256
F32 = jnp.float32
BF16 = jnp.bfloat16


def pairs(count, first):
    swaps = {}
    for low in range(first, count - 1, 2):
        swaps[low], swaps[low + 1] = low + 1, low
    return [(i, swaps.get(i, i)) for i in range(count)]


def swap(one, two, axis):
    count = lax.axis_size(axis)
    return lax.ppermute(one, axis, pairs(count, 0)), lax.ppermute(two, axis, pairs(count, 1))


def call(kernel, outs, *args, scratch=(), smem=1, after=()):
    vmem = pl.BlockSpec(memory_space=pltpu.VMEM)
    specs = [pl.BlockSpec(memory_space=pltpu.SMEM)] * smem + [vmem] * (len(args) - smem)
    specs += [pl.BlockSpec(memory_space=pl.ANY)] * len(after)
    used = len(args)
    held = sum(math.prod(s.shape) * 4 for s in scratch)

    def body(*refs):
        kernel(*refs[:used], *refs[used + len(after) :])

    return pl.pallas_call(
        body,
        out_shape=[jax.ShapeDtypeStruct(s, F32) for s in outs],
        in_specs=specs,
        out_specs=[vmem] * len(outs),
        scratch_shapes=list(scratch),
        compiler_params=pltpu.CompilerParams(vmem_limit_bytes=held + 6 * 1024 * 1024),
    )(*args, *after)


class Side:
    def __init__(self, index, count):
        self.even = index % 2 == 0
        self.has_below = index > 0
        self.has_above = index < count - 1
        self.one_valid = jnp.where(self.even, self.has_above, self.has_below)
        self.two_valid = jnp.where(self.even, self.has_below, self.has_above)

    def one(self, above, below):
        return jnp.where(self.even, above, below)

    def two(self, above, below):
        return jnp.where(self.even, below, above)


def rows_of(start, size):
    return pl.ds(pl.multiple_of(start, 8), size)


def lane_of(shape):
    return lax.broadcasted_iota(jnp.int32, shape, 1)


def group_of(count, width):
    return -(-count // (LANES // width))


def pack(load, count, rows, width, src, out):
    each = group_of(count, width)
    lane = lane_of((rows, LANES))

    def member(j, carry):
        value = jnp.zeros((rows, LANES), F32)
        for g in range(-(-count // each)):
            x = jnp.minimum(g * each + j, count - 1)
            turned = pltpu.roll(load(x), (g * width - src + LANES) % LANES, 1)
            value = jnp.where((lane >= g * width) & (lane < (g + 1) * width), turned, value)
        out[rows_of(j * rows, rows), :] = value
        return carry

    lax.fori_loop(0, each, member, 0, unroll=min(each, 8))


def unpack(ref, x, count, rows, width, dst, valid):
    each = group_of(count, width)
    g, j = x // each, x % each
    turned = pltpu.roll(ref[rows_of(j * rows, rows), :], (dst - g * width + LANES) % LANES, 1)
    away = (lane_of((rows, LANES)) - dst + LANES) % LANES
    return jnp.where((away < width) & valid, turned, 0.0)


def split(value):
    high = value.astype(BF16)
    return high, (value - high.astype(F32)).astype(BF16)


def stack_rows(value):
    high, low = split(value)
    return jnp.concatenate([high, high, low], axis=0)


def dot(a, b):
    return jnp.dot(a, b, preferred_element_type=F32)


def dot_nt(a, b):
    return lax.dot_general(a, b, (((1,), (1,)), ((), ())), preferred_element_type=F32)


def first_slabs(info, *refs, ny, ov):
    parts, (one, two) = refs[:-2], refs[-2:]
    side = Side(info[1], ny)
    cx, cy, _ = parts[0].shape
    for k, part in enumerate(parts):
        one[k * cx : (k + 1) * cx] = part[:, rows_of(side.one(cy - ov, 0), ov), :]
        two[k * cx : (k + 1) * cx] = part[:, rows_of(side.two(cy - ov, 0), ov), :]


def second_slabs(info, *refs, ny, nz, ov):
    parts, (got_one, got_two, field, coef, one, two) = refs[:-6], refs[-6:]
    side, along = Side(info[1], ny), Side(info[2], nz)
    cx, cy, cz = parts[0].shape
    ey = cy + 2 * ov
    count = (len(parts) - 1) * cx
    for k, part in enumerate(parts):
        out, first = (coef, 0) if k == len(parts) - 1 else (field, k * cx)

        def place(x, carry, k=k, part=part, out=out, first=first):
            a = got_one[k * cx + x]
            b = got_two[k * cx + x]
            row = (first + x) * ey
            above = jnp.where(side.even, a, b)
            below = jnp.where(side.even, b, a)
            out[rows_of(row, ov), :] = jnp.where(side.has_below, below, 0.0)
            out[rows_of(row + ov, cy), :] = part[x]
            out[rows_of(row + ov + cy, ov), :] = jnp.where(side.has_above, above, 0.0)
            return carry

        lax.fori_loop(0, cx, place, 0, unroll=8)

    edge = group_of(count, ov) * ey
    for ref, planes, first in ((field, count, 0), (coef, cx, edge)):

        def load(x, ref=ref):
            return ref[rows_of(x * ey, ey), :]

        last = first + group_of(planes, ov) * ey
        pack(load, planes, ey, ov, along.one(cz - ov, 0), one.at[first:last])
        pack(load, planes, ey, ov, along.two(cz - ov, 0), two.at[first:last])


def extended(field, got_one, got_two, x, count, ey, ov, along):
    halo = unpack(got_one, x, count, ey, ov, along.one(0, LANES - ov), along.one_valid)
    halo = halo + unpack(got_two, x, count, ey, ov, along.two(0, LANES - ov), along.two_valid)
    return jnp.concatenate([field[rows_of(x * ey, ey), :], halo], axis=1)


def turn(value):
    group = LANES // 8
    row = lax.broadcasted_iota(jnp.int32, (8, LANES), 0)
    column = lane_of((8, LANES)) // group
    for bit in (4, 2, 1):
        up = pltpu.roll(pltpu.roll(value, 8 - bit, 0), bit * group, 1)
        down = pltpu.roll(pltpu.roll(value, bit, 0), LANES - bit * group, 1)
        moved = jnp.where((row & bit) == 0, up, down)
        value = jnp.where((row & bit) == (column & bit), value, moved)
    return value


def solve(source, store, tables, state, count, back, ey):
    zt, y_on, y_back, x_on, x_back, recip = tables
    s0, s1 = state
    z_high, z_low = split(zt[...])
    modes = recip.shape[1]
    group = LANES // 8
    lane = lane_of((ey, LANES))
    octs = ey // 8
    nothing = jnp.zeros((ey, LANES), F32)

    def times_y(table, core, side):
        two = 2 * ey
        first = dot(table[...], stack_rows(jnp.concatenate([core[:two], core[two : 2 * two]], axis=1)))
        second = dot(table[...], stack_rows(jnp.concatenate([core[2 * two : 3 * two], core[3 * two :]], axis=1)))
        third = dot(table[...], stack_rows(jnp.concatenate([side, nothing], axis=0)))
        return jnp.concatenate([first[:, :LANES], first[:, LANES:], second[:, :LANES], second[:, LANES:]], axis=0), third[:ey]

    def on(k, carry):
        high, low = split(jnp.concatenate([source(8 * k + j) for j in range(8)], axis=0))
        value = dot(high, z_high) + (dot(high, z_low) + dot(low, z_high))
        side = nothing
        for j in range(8):
            turned = pltpu.roll(value[j * ey : (j + 1) * ey, LANES:], j * group, 1)
            side = jnp.where(lane // group == j, turned, side)
        core, side = times_y(y_on, value[:, :LANES], side)
        s0[rows_of(k * 8 * ey, 8 * ey), :] = core
        for q in range(octs):
            s1[rows_of(q * count + k * 8, 8), :] = turn(side[q * 8 : (q + 1) * 8])
        return carry

    lax.fori_loop(0, count // 8, on, 0, unroll=3)

    def times_x(value, factor):
        value = dot(x_on[...], stack_rows(value))
        value = jnp.concatenate([value[i * modes : (i + 1) * modes] * factor for i in range(value.shape[0] // modes)], axis=0)
        return dot(x_back[...], stack_rows(value))[:back]

    def middle(h, carry):
        q = 2 * h
        value = [s0[pl.ds(q + i, count, stride=ey), :] for i in range(2)]
        value = times_x(jnp.concatenate(value, axis=1), jnp.concatenate([recip[q], recip[q + 1]], axis=1))
        for i in range(2):
            s0[pl.ds(q + i, back, stride=ey), :] = value[:, i * LANES : (i + 1) * LANES]
        return carry

    for q in range(octs):
        value = times_x(s1[q * count : (q + 1) * count, :], recip[ey + q])
        s1[q * count : q * count + back, :] = value
    lax.fori_loop(0, ey // 2, middle, 0, unroll=10)

    def off(k, carry):
        side = jnp.concatenate([turn(s1[rows_of(q * count + k * 8, 8), :]) for q in range(octs)], axis=0)
        core, side = times_y(y_back, s0[rows_of(k * 8 * ey, 8 * ey), :], side)
        side = jnp.concatenate([side] + [pltpu.roll(side, LANES - j * group, 1) for j in range(1, 8)], axis=0)
        high, low = split(jnp.concatenate([core, side], axis=1))
        value = dot_nt(high, z_high) + (dot_nt(high, z_low) + dot_nt(low, z_high))
        for j in range(8):
            store(8 * k + j, value[j * ey : (j + 1) * ey])
        return carry

    lax.fori_loop(0, back // 8, off, 0, unroll=2 if back % 16 == 0 else 3)


def merged(core, halo, low):
    lane = lane_of(core.shape)
    return jnp.where((lane < LANES // 2) == low, core, halo)


def first_solve(info, field, got_one, got_two, zt, y_on, y_back, x_on, x_back, recip, u, block, rest, one, two, s0, s1, *, nz, ov, ey, cz):
    along = Side(info[2], nz)
    count = field.shape[0] // ey
    w = 2 * ov + 1
    edge, half = group_of(count, ov) * ey, rest.shape[0] // 2
    rest[:half] = got_one[edge:]
    rest[half:] = got_two[edge:]

    def source(x):
        value = extended(field, got_one, got_two, x, count, ey, ov, along)
        block[rows_of(x * ey, ey), :] = value
        return value

    def store(x, value):
        u[rows_of(x * ey, ey), :] = value

    solve(source, store, (zt, y_on, y_back, x_on, x_back, recip), (s0, s1), count, count, ey)

    for out, low in ((one, ~along.even), (two, along.even)):

        def load(x, low=low):
            rows = rows_of(x * ey, ey)
            return merged(u[rows, :LANES], u[rows, LANES:], low)

        pack(load, count, ey, w, jnp.where(low, LANES - ov, cz - ov - 1), out)


def sum_z(info, u, got_one, got_two, core_out, rest_out, one, two, *, ny, nz, ov, ey, cz):
    side, along = Side(info[1], ny), Side(info[2], nz)
    count = u.shape[0] // ey
    w = 2 * ov + 1
    lane = lane_of((ey, LANES))
    inside = ((lane <= ov) & along.has_above) | ((lane >= LANES - ov - 1) & along.has_below)

    def add(x, carry):
        rows = rows_of(x * ey, ey)
        core, rest = u[rows, :LANES], u[rows, LANES:]
        for got, low, valid in ((got_one, ~along.even, along.one_valid), (got_two, along.even, along.two_valid)):
            part = unpack(got, x, count, ey, w, jnp.where(low, LANES - ov - 1, cz - ov), valid)
            mine = (lane < LANES // 2) == low
            core, rest = core + jnp.where(mine, part, 0.0), rest + jnp.where(mine, 0.0, part)
        core_out[rows, :] = core
        rest_out[rows, :] = jnp.where(inside, rest, 0.0)
        return carry

    lax.fori_loop(0, count, add, 0, unroll=8)
    tall, halo = 2 * ov, 2 * (ov + 1)
    each = group_of(count, halo)
    for out, high in ((one, side.even), (two, ~side.even)):
        start = jnp.where(high, ey - tall, 0)
        odd = pl.ds(jnp.where(high, ey - tall - 1, tall), count, stride=ey)

        def main(x, carry, out=out, start=start):
            out[rows_of(x * tall, tall), :] = core_out[rows_of(x * ey + start, tall), :]
            return carry

        lax.fori_loop(0, count, main, 0, unroll=8)
        base = count * tall

        def load(x, start=start):
            return rest_out[rows_of(x * ey + start, tall), :]

        pack(load, count, tall, halo, LANES - ov - 1, out.at[base : base + each * tall])
        base = base + each * tall
        out[base : base + count, :] = core_out[odd, :]
        out[base + count : base + 2 * count, :] = rest_out[odd, :]


def coefficients(info, *refs, nz, ov, ey):
    parts, out = refs[:-1], refs[-1]
    along = Side(info[2], nz)
    half = len(parts) // 2
    cx = parts[0].shape[0] // ey
    for k in range(half):
        core, rest = parts[k], parts[half + k]
        edge = rest.shape[0] // 2

        def plane(x, carry, k=k, core=core, rest=rest, edge=edge):
            value = extended(core, rest.at[:edge], rest.at[edge:], x, cx, ey, ov, along)
            out[rows_of((k * cx + x) * ey, ey), :] = value + 5.0
            return carry

        lax.fori_loop(0, cx, plane, 0, unroll=4)


def second_solve(info, core_in, rest_in, got_one, got_two, block, coef, zt, y_on, y_back, x_on, x_back, recip, u, first, one, two, s0, s1, core_v, rest_v, far, *, ny, nz, ov, ey, cx, cz):
    side, along = Side(info[1], ny), Side(info[2], nz)
    count = coef.shape[0] // ey
    tall, halo = 2 * ov, 2 * (ov + 1)
    each = group_of(count, halo)
    room = ey + 2 * ov
    cy = ey - 2 * ov
    main_rows = count * tall
    odd_rows = main_rows + each * tall

    def sides(a, b):
        a, b = jnp.where(side.one_valid, a, 0.0), jnp.where(side.two_valid, b, 0.0)
        return jnp.where(side.even, b, a), jnp.where(side.even, a, b)

    def gather(x, carry):
        rows, slab = rows_of(x * ey, ey), rows_of(x * tall, tall)
        for source, out, (a, b) in (
            (core_in, core_v, (got_one[slab, :], got_two[slab, :])),
            (
                rest_in,
                rest_v,
                [unpack(got.at[main_rows:odd_rows], x, count, tall, halo, LANES - ov - 1, True) for got in (got_one, got_two)],
            ),
        ):
            below, above = sides(a, b)
            value = source[rows, :]
            low, high = value[:tall] + below, value[ey - tall :] + above
            out[rows_of(x * room + ov, ov), :] = jnp.where(side.has_below, low[:ov], 0.0)
            out[rows_of(x * room + tall, ov), :] = low[ov:]
            out[rows_of(x * room + ov + tall, ey - 2 * tall), :] = value[tall : ey - tall]
            out[rows_of(x * room + ov + ey - tall, ov), :] = high[:ov]
            out[rows_of(x * room + ey, ov), :] = jnp.where(side.has_above, high[ov:], 0.0)
        return carry

    lax.fori_loop(0, count, gather, 0, unroll=4)
    for out, start in ((core_v, odd_rows), (rest_v, odd_rows + count)):
        below, above = sides(got_one[start : start + count, :], got_two[start : start + count, :])
        out[pl.ds(ov - 1, count, stride=room), :] = below
        out[pl.ds(ov + ey, count, stride=room), :] = above

    lane = lane_of((ey, RING))
    y = lax.broadcasted_iota(jnp.int32, (ey, RING), 0)
    inside = (lane < cz) | ((lane < cz + ov) & along.has_above) | ((lane >= RING - ov) & along.has_below)
    inside = inside & ((y >= ov) | side.has_below) & ((y < ey - ov) | side.has_above)

    def plane(x):
        at = (info[0] * cx + x) % count
        before, after = jnp.where(at > 0, 1.0, 0.0), jnp.where(at < count - 1, 1.0, 0.0)
        spots = [(x + shift) % count * room + ov for shift in (0, count - 1, 1)]
        halves = []
        for ref in (core_v, rest_v):
            mid, left, right = [ref[rows_of(spot, ey), :] for spot in spots]
            mid_y, left_y, right_y = [ref[pl.ds(spot - 1, ey), :] + ref[pl.ds(spot + 1, ey), :] for spot in spots]
            across, corner = before * left + after * right, before * left_y + after * right_y
            faces = mid_y + across
            halves.append((mid, 0.5 * faces + 0.125 * corner, 0.5 * mid + 0.125 * faces + 0.0625 * corner))
        mid, flat, slope = [jnp.concatenate(pair, axis=1) for pair in zip(*halves)]
        rows = rows_of(x * ey, ey)
        value = block[rows, :] - coef[rows, :] * mid + flat + (pltpu.roll(slope, 1, 1) + pltpu.roll(slope, RING - 1, 1))
        return jnp.where(inside, value, 0.0)

    def store(x, value):
        rows = rows_of(x * ey, ey)
        u[rows, :] = value[:, :LANES]
        far[rows, :] = value[:, LANES:]

    solve(plane, store, (zt, y_on, y_back, x_on, x_back, recip), (s0, s1), count, cx, ey)

    def load(x):
        return far[rows_of(x * ey, ey), :]

    pack(load, cx, ey, ov, along.one(0, LANES - ov), one)
    pack(load, cx, ey, ov, along.two(0, LANES - ov), two)

    def keep(x, carry):
        first[rows_of(x * cy, cy), :] = core_v[rows_of(x * room + 2 * ov, cy), :]
        return carry

    lax.fori_loop(0, cx, keep, 0, unroll=8)


def last_sum_z(info, u, got_one, got_two, v, one, two, *, ny, nz, ov, ey, cx, cz):
    side, along = Side(info[1], ny), Side(info[2], nz)

    def add(x, carry):
        rows = rows_of(x * ey, ey)
        value = u[rows, :]
        value = value + unpack(got_one, x, cx, ey, ov, along.one(cz - ov, 0), along.one_valid)
        value = value + unpack(got_two, x, cx, ey, ov, along.two(cz - ov, 0), along.two_valid)
        v[rows, :] = value
        one[rows_of(x * ov, ov), :] = v[rows_of(x * ey + side.one(ey - ov, 0), ov), :]
        two[rows_of(x * ov, ov), :] = v[rows_of(x * ey + side.two(ey - ov, 0), ov), :]
        return carry

    lax.fori_loop(0, cx, add, 0, unroll=8)


def last_sum_y(info, v, got_one, got_two, first, out, *, ny, ov, ey, cx):
    side = Side(info[1], ny)
    cy = ey - 2 * ov

    def add(x, carry):
        a, b = got_one[rows_of(x * ov, ov), :], got_two[rows_of(x * ov, ov), :]
        above, below = jnp.where(side.even, a, b), jnp.where(side.even, b, a)
        above, below = jnp.where(side.has_above, above, 0.0), jnp.where(side.has_below, below, 0.0)
        value = v[rows_of(x * ey + ov, cy), :] + first[rows_of(x * cy, cy), :]
        out[x] = jnp.concatenate([value[:ov] + below, value[ov : cy - ov], value[cy - ov :] + above], axis=0)
        return carry

    lax.fori_loop(0, cx, add, 0, unroll=8)


def reciprocals(eigen_x, rest, out):
    def row(q, carry):
        out[q] = 1.0 / (eigen_x[...] + rest[pl.ds(q, 1), :])
        return carry

    lax.fori_loop(0, out.shape[0], row, 0, unroll=5)


def gather_x(block):
    count = lax.axis_size("gx")
    parts = [block]
    for shift in range(1, count):
        parts.append(lax.ppermute(block, "gx", [((i + shift) % count, i) for i in range(count)]))
    return parts


def columns(table):
    high = lax.reduce_precision(table, 8, 7)
    return jnp.concatenate([high, table - high, high], axis=1).astype(BF16)


def local(right_side, reaction, basis_x, basis_y, basis_z, eigen_x, eigen_y, eigen_z):
    cx, cy, cz = right_side.shape
    ex, ey, ez = basis_x.shape[0], basis_y.shape[0], basis_z.shape[0]
    ov = (ex - cx) // 2
    nx, ny, nz = lax.axis_size("gx"), lax.axis_size("gy"), lax.axis_size("gz")
    ix, iy, iz = lax.axis_index("gx"), lax.axis_index("gy"), lax.axis_index("gz")
    count = nx * cx
    info = jnp.stack([ix, iy, iz]).astype(jnp.int32)
    w, tall, halo = 2 * ov + 1, 2 * ov, 2 * (ov + 1)
    at = dict(ov=ov, ey=ey, cz=cz)

    f_parts = gather_x(right_side)

    blocks = [jnp.pad(basis_x.T, ((0, 0), (i * cx, (nx - 1 - i) * cx)))[:, ov : ov + count] for i in range(nx)]
    table = jnp.concatenate(blocks, axis=0)
    table = lax.dynamic_slice_in_dim(jnp.concatenate([table, table], axis=1), ix * cx, count, axis=1)
    zero = jnp.zeros((ey, ey), F32)
    double = jnp.concatenate([jnp.concatenate([basis_y, zero], axis=1), jnp.concatenate([zero, basis_y], axis=1)], axis=0)
    zt = jnp.concatenate([basis_z[ov:], jnp.zeros((RING - ez, ez), F32), basis_z[:ov]], axis=0)
    zt = jnp.pad(zt, ((0, 0), (0, RING - ez)))
    rest = eigen_y[:, None] + eigen_z[None, :]
    rest = jnp.concatenate([rest[:, :LANES], rest[:, LANES:].reshape(-1, LANES)], axis=0)
    recip = call(reciprocals, [(rest.shape[0], ex, LANES)], jnp.broadcast_to(eigen_x[:, None], (ex, LANES)), rest, smem=0)[0]
    tables = (zt, columns(double.T), columns(double), columns(table), columns(table.T), recip)

    slabs = call(functools.partial(first_slabs, ny=ny, ov=ov), [(count + cx, ov, cz)] * 2, info, *f_parts, reaction)
    got = swap(*slabs, "gy")
    edge = group_of(cx, ov) * ey
    small = (group_of(count, ov) * ey + edge, LANES)
    f, c, *slabs = call(
        functools.partial(second_slabs, ny=ny, nz=nz, ov=ov), [(count * ey, cz), (cx * ey, cz), small, small], info, *f_parts, reaction, *got
    )
    got = swap(*slabs, "gz")
    c_parts = gather_x(c)
    state = [pltpu.VMEM((count * ey, LANES), F32), pltpu.VMEM((ey // 8 * count, LANES), F32)]
    small = (group_of(count, w) * ey, LANES)
    u, block, rest, *slabs = call(
        functools.partial(first_solve, nz=nz, **at), [(count * ey, RING)] * 2 + [(2 * edge, LANES), small, small], info, f, *got, *tables, scratch=state
    )
    got = swap(*slabs, "gz")
    c_parts += gather_x(rest)
    tall_rows = (count * tall + group_of(count, halo) * tall + 2 * count, LANES)
    core, rest, *slabs = call(functools.partial(sum_z, ny=ny, nz=nz, **at), [(count * ey, LANES)] * 2 + [tall_rows, tall_rows], info, u, *got)
    got = swap(*slabs, "gy")
    c = call(functools.partial(coefficients, nz=nz, ov=ov, ey=ey), [(count * ey, RING)], info, *c_parts, after=slabs[:1])[0]
    small = (group_of(cx, ov) * ey, LANES)
    state += [pltpu.VMEM((count * (ey + 2 * ov), LANES), F32)] * 2 + [pltpu.VMEM((cx * ey, LANES), F32)]
    u, first, *slabs = call(
        functools.partial(second_solve, ny=ny, nz=nz, cx=cx, **at),
        [(cx * ey, LANES), (cx * cy, LANES), small, small], info, core, rest, *got, block, c, *tables, scratch=state,
    )
    got = swap(*slabs, "gz")
    v, *slabs = call(functools.partial(last_sum_z, ny=ny, nz=nz, cx=cx, **at), [(cx * ey, LANES)] + [(cx * ov, LANES)] * 2, info, u, *got)
    got = swap(*slabs, "gy")
    return call(functools.partial(last_sum_y, ny=ny, ov=ov, ey=ey, cx=cx), [(cx, cy, cz)], info, v, *got, first)[0]


def solution(mesh):
    return jax.shard_map(
        local,
        mesh=mesh,
        in_specs=(P("gx", "gy", "gz"), P("gx", "gy", "gz"), P(), P(), P(), P(), P(), P()),
        out_specs=P("gx", "gy", "gz"),
        check_vma=False,
    )
```

```python
import functools
import math

import jax
import jax.numpy as jnp
from jax import lax
from jax.experimental import pallas as pl
from jax.experimental.pallas import tpu as pltpu
from jax.sharding import PartitionSpec as P


LANES = 128
RING = 256
F32 = jnp.float32
BF16 = jnp.bfloat16


def pairs(count, first):
    swaps = {}
    for low in range(first, count - 1, 2):
        swaps[low], swaps[low + 1] = low + 1, low
    return [(i, swaps.get(i, i)) for i in range(count)]


def swap(one, two, axis):
    count = lax.axis_size(axis)
    return lax.ppermute(one, axis, pairs(count, 0)), lax.ppermute(two, axis, pairs(count, 1))


def call(kernel, outs, *args, scratch=(), smem=1, after=()):
    vmem = pl.BlockSpec(memory_space=pltpu.VMEM)
    specs = [pl.BlockSpec(memory_space=pltpu.SMEM)] * smem + [vmem] * (len(args) - smem)
    specs += [pl.BlockSpec(memory_space=pl.ANY)] * len(after)
    used = len(args)
    held = sum(math.prod(s.shape) * 4 for s in scratch)

    def body(*refs):
        kernel(*refs[:used], *refs[used + len(after) :])

    return pl.pallas_call(
        body,
        out_shape=[jax.ShapeDtypeStruct(s[:2], BF16) if BF16 in s else jax.ShapeDtypeStruct(s, F32) for s in outs],
        in_specs=specs,
        out_specs=[vmem] * len(outs),
        scratch_shapes=list(scratch),
        compiler_params=pltpu.CompilerParams(vmem_limit_bytes=held + 6 * 1024 * 1024),
    )(*args, *after)


class Side:
    def __init__(self, index, count):
        self.even = index % 2 == 0
        self.has_below = index > 0
        self.has_above = index < count - 1
        self.one_valid = jnp.where(self.even, self.has_above, self.has_below)
        self.two_valid = jnp.where(self.even, self.has_below, self.has_above)

    def one(self, above, below):
        return jnp.where(self.even, above, below)

    def two(self, above, below):
        return jnp.where(self.even, below, above)


def rows_of(start, size):
    return pl.ds(pl.multiple_of(start, 8), size)


def lane_of(shape):
    return lax.broadcasted_iota(jnp.int32, shape, 1)


def group_of(count, width):
    return -(-count // (LANES // width))


def pack(load, count, rows, width, src, out):
    each = group_of(count, width)
    lane = lane_of((rows, LANES))

    def member(j, carry):
        value = jnp.zeros((rows, LANES), F32)
        for g in range(-(-count // each)):
            x = jnp.minimum(g * each + j, count - 1)
            turned = pltpu.roll(load(x), (g * width - src + LANES) % LANES, 1)
            value = jnp.where((lane >= g * width) & (lane < (g + 1) * width), turned, value)
        out[rows_of(j * rows, rows), :] = value
        return carry

    lax.fori_loop(0, each, member, 0, unroll=min(each, 8))


def unpack(ref, x, count, rows, width, dst, valid):
    each = group_of(count, width)
    g, j = x // each, x % each
    turned = pltpu.roll(ref[rows_of(j * rows, rows), :], (dst - g * width + LANES) % LANES, 1)
    away = (lane_of((rows, LANES)) - dst + LANES) % LANES
    return jnp.where((away < width) & valid, turned, 0.0)


def split(value):
    high = value.astype(BF16)
    return high, (value - high.astype(F32)).astype(BF16)


def stack_rows(value):
    high, low = split(value)
    return jnp.concatenate([high, high, low], axis=0)


def dot(a, b):
    return jnp.dot(a, b, preferred_element_type=F32)


def first_slabs(info, *refs, ny, ov):
    parts, (one, two) = refs[:-2], refs[-2:]
    side = Side(info[1], ny)
    cx, cy, _ = parts[0].shape
    for k, part in enumerate(parts):
        one[k * cx : (k + 1) * cx] = part[:, rows_of(side.one(cy - ov, 0), ov), :]
        two[k * cx : (k + 1) * cx] = part[:, rows_of(side.two(cy - ov, 0), ov), :]


def second_slabs(info, *refs, ny, nz, ov):
    parts, (got_one, got_two, field, coef, one, two) = refs[:-6], refs[-6:]
    side, along = Side(info[1], ny), Side(info[2], nz)
    cx, cy, cz = parts[0].shape
    ey = cy + 2 * ov
    count = (len(parts) - 1) * cx
    for k, part in enumerate(parts):
        out, first = (coef, 0) if k == len(parts) - 1 else (field, k * cx)

        def place(x, carry, k=k, part=part, out=out, first=first):
            a = got_one[k * cx + x]
            b = got_two[k * cx + x]
            row = (first + x) * ey
            above = jnp.where(side.even, a, b)
            below = jnp.where(side.even, b, a)
            out[rows_of(row, ov), :] = jnp.where(side.has_below, below, 0.0)
            out[rows_of(row + ov, cy), :] = part[x]
            out[rows_of(row + ov + cy, ov), :] = jnp.where(side.has_above, above, 0.0)
            return carry

        lax.fori_loop(0, cx, place, 0, unroll=8)

    edge = group_of(count, ov) * ey
    for ref, planes, first in ((field, count, 0), (coef, cx, edge)):

        def load(x, ref=ref):
            return ref[rows_of(x * ey, ey), :]

        last = first + group_of(planes, ov) * ey
        pack(load, planes, ey, ov, along.one(cz - ov, 0), one.at[first:last])
        pack(load, planes, ey, ov, along.two(cz - ov, 0), two.at[first:last])


def extended(field, got_one, got_two, x, count, ey, ov, along):
    halo = unpack(got_one, x, count, ey, ov, along.one(0, LANES - ov), along.one_valid)
    halo = halo + unpack(got_two, x, count, ey, ov, along.two(0, LANES - ov), along.two_valid)
    return jnp.concatenate([field[rows_of(x * ey, ey), :], halo], axis=1)


def turn(value):
    group = LANES // 8
    row = lax.broadcasted_iota(jnp.int32, (8, LANES), 0)
    column = lane_of((8, LANES)) // group
    for bit in (4, 2, 1):
        up = pltpu.roll(pltpu.roll(value, 8 - bit, 0), bit * group, 1)
        down = pltpu.roll(pltpu.roll(value, bit, 0), LANES - bit * group, 1)
        moved = jnp.where((row & bit) == 0, up, down)
        value = jnp.where((row & bit) == (column & bit), value, moved)
    return value


def solve(source, store, tables, state, count, back, ey, cx):
    z_on, z_back, y_on, y_back, x_on, x_back, recip = tables
    s0, s1 = state
    modes = recip.shape[1]
    group = LANES // 8
    lane = lane_of((ey, LANES))
    octs = ey // 8
    nothing = jnp.zeros((ey, LANES), F32)

    def times_y(table, core, sides):
        planes = [core[j * ey : (j + 1) * ey] for j in range(cx)] + sides
        planes += [nothing] * (-len(planes) % 4)
        done = []
        for j in range(0, len(planes), 4):
            quad = jnp.concatenate([jnp.concatenate(planes[j + i : j + i + 2], axis=0) for i in (0, 2)], axis=1)
            quad = dot(table[...], stack_rows(quad))
            done += [quad[i * ey : (i + 1) * ey, k * LANES : (k + 1) * LANES] for k in range(2) for i in range(2)]
        return done[:cx], done[cx : cx + len(sides)]

    def on(part, carry):
        rows = []
        for j in range(cx):
            value = source(part * cx + j)
            high, low = split(value[:, :LANES])
            near = value[:, LANES:].astype(BF16).astype(F32)
            halo = near + pltpu.roll(value[:, LANES:] - near, group, 1) + pltpu.roll(near, 2 * group, 1)
            rows.append((high, low, high, halo.astype(BF16)))
        value = dot(jnp.concatenate([jnp.concatenate(piece, axis=0) for piece in zip(*rows)], axis=1), z_on[...])
        sides = []
        for k in range(cx // 8):
            side = nothing
            for j in range(8):
                turned = pltpu.roll(value[(8 * k + j) * ey : (8 * k + j + 1) * ey, LANES:], j * group, 1)
                side = jnp.where(lane // group == j, turned, side)
            sides.append(side)
        core, sides = times_y(y_on, value[:, :LANES], sides)
        for j in range(cx):
            s0[rows_of((part * cx + j) * ey, ey), :] = core[j]
        for k in range(cx // 8):
            for q in range(octs):
                s1[rows_of(q * count + part * cx + k * 8, 8), :] = turn(sides[k][q * 8 : (q + 1) * 8])
        return carry

    lax.fori_loop(0, count // cx, on, 0, unroll=2)

    def times_x(value, factor):
        value = dot(x_on[...], stack_rows(value))
        value = jnp.concatenate([value[i * modes : (i + 1) * modes] * factor for i in range(value.shape[0] // modes)], axis=0)
        return dot(x_back[...], stack_rows(value))[:back]

    def middle(h, carry):
        q = 2 * h
        value = [s0[pl.ds(q + i, count, stride=ey), :] for i in range(2)]
        value = times_x(jnp.concatenate(value, axis=1), jnp.concatenate([recip[q], recip[q + 1]], axis=1))
        for i in range(2):
            s0[pl.ds(q + i, back, stride=ey), :] = value[:, i * LANES : (i + 1) * LANES]
        return carry

    for q in range(octs):
        value = times_x(s1[q * count : (q + 1) * count, :], recip[ey + q])
        s1[q * count : q * count + back, :] = value
    lax.fori_loop(0, ey // 2, middle, 0, unroll=20)

    def off(part, carry):
        sides = []
        for k in range(cx // 8):
            sides.append(jnp.concatenate([turn(s1[rows_of(q * count + part * cx + k * 8, 8), :]) for q in range(octs)], axis=0))
        core, sides = times_y(y_back, s0[rows_of(part * cx * ey, cx * ey), :], sides)
        rows = []
        for k in range(cx // 8):
            near = sides[k].astype(BF16).astype(F32)
            far = sides[k] - near
            for j in range(8):
                high, low = split(core[8 * k + j])
                halo = [pltpu.roll(piece, (i - j) * group % LANES, 1) for i, piece in enumerate((near, far, near))]
                halo = jnp.where(lane < group, halo[0], jnp.where(lane < 2 * group, halo[1], halo[2]))
                rows.append((high, low, high, halo.astype(BF16)))
        value = dot(jnp.concatenate([jnp.concatenate(piece, axis=0) for piece in zip(*rows)], axis=1), z_back[...])
        for j in range(cx):
            store(part * cx + j, value[j * ey : (j + 1) * ey])
        return carry

    lax.fori_loop(0, back // cx, off, 0, unroll=2 if back > cx else 1)


def merged(core, halo, low):
    lane = lane_of(core.shape)
    return jnp.where((lane < LANES // 2) == low, core, halo)


def first_solve(info, field, got_one, got_two, z_on, z_back, y_on, y_back, x_on, x_back, recip, u, block, rest, one, two, s0, s1, *, nz, ov, ey, cx, cz):
    along = Side(info[2], nz)
    count = field.shape[0] // ey
    w = 2 * ov + 1
    edge, half = group_of(count, ov) * ey, rest.shape[0] // 2
    rest[:half] = got_one[edge:]
    rest[half:] = got_two[edge:]

    def source(x):
        value = extended(field, got_one, got_two, x, count, ey, ov, along)
        block[rows_of(x * ey, ey), :] = value
        return value

    def store(x, value):
        u[rows_of(x * ey, ey), :] = value

    solve(source, store, (z_on, z_back, y_on, y_back, x_on, x_back, recip), (s0, s1), count, count, ey, cx)

    for out, low in ((one, ~along.even), (two, along.even)):

        def load(x, low=low):
            rows = rows_of(x * ey, ey)
            return merged(u[rows, :LANES], u[rows, LANES:], low)

        pack(load, count, ey, w, jnp.where(low, LANES - ov, cz - ov - 1), out)


def sum_z(info, u, got_one, got_two, core_out, rest_out, one, two, *, ny, nz, ov, ey, cz):
    side, along = Side(info[1], ny), Side(info[2], nz)
    count = u.shape[0] // ey
    w = 2 * ov + 1
    lane = lane_of((ey, LANES))
    inside = ((lane <= ov) & along.has_above) | ((lane >= LANES - ov - 1) & along.has_below)

    def add(x, carry):
        rows = rows_of(x * ey, ey)
        core, rest = u[rows, :LANES], u[rows, LANES:]
        for got, low, valid in ((got_one, ~along.even, along.one_valid), (got_two, along.even, along.two_valid)):
            part = unpack(got, x, count, ey, w, jnp.where(low, LANES - ov - 1, cz - ov), valid)
            mine = (lane < LANES // 2) == low
            core, rest = core + jnp.where(mine, part, 0.0), rest + jnp.where(mine, 0.0, part)
        core_out[rows, :] = core
        rest_out[rows, :] = jnp.where(inside, rest, 0.0)
        return carry

    lax.fori_loop(0, count, add, 0, unroll=8)
    tall, halo = 2 * ov, 2 * (ov + 1)
    each = group_of(count, halo)
    for out, high in ((one, side.even), (two, ~side.even)):
        start = jnp.where(high, ey - tall, 0)
        odd = pl.ds(jnp.where(high, ey - tall - 1, tall), count, stride=ey)

        def main(x, carry, out=out, start=start):
            out[rows_of(x * tall, tall), :] = core_out[rows_of(x * ey + start, tall), :]
            return carry

        lax.fori_loop(0, count, main, 0, unroll=8)
        base = count * tall

        def load(x, start=start):
            return rest_out[rows_of(x * ey + start, tall), :]

        pack(load, count, tall, halo, LANES - ov - 1, out.at[base : base + each * tall])
        base = base + each * tall
        out[base : base + count, :] = core_out[odd, :]
        out[base + count : base + 2 * count, :] = rest_out[odd, :]


def coefficients(info, *refs, nz, ov, ey):
    parts, out = refs[:-1], refs[-1]
    along = Side(info[2], nz)
    half = len(parts) // 2
    cx = parts[0].shape[0] // ey
    for k in range(half):
        core, rest = parts[k], parts[half + k]
        edge = rest.shape[0] // 2

        def plane(x, carry, k=k, core=core, rest=rest, edge=edge):
            value = extended(core, rest.at[:edge], rest.at[edge:], x, cx, ey, ov, along)
            out[rows_of((k * cx + x) * ey, ey), :] = value + 5.0
            return carry

        lax.fori_loop(0, cx, plane, 0, unroll=4)


def second_solve(info, core_in, rest_in, got_one, got_two, block, coef, z_on, z_back, y_on, y_back, x_on, x_back, recip, u, first, one, two, s0, s1, core_v, rest_v, far, *, ny, nz, ov, ey, cx, cz):
    side, along = Side(info[1], ny), Side(info[2], nz)
    count = coef.shape[0] // ey
    tall, halo = 2 * ov, 2 * (ov + 1)
    each = group_of(count, halo)
    room = ey + 2 * ov
    cy = ey - 2 * ov
    main_rows = count * tall
    odd_rows = main_rows + each * tall

    def sides(a, b):
        a, b = jnp.where(side.one_valid, a, 0.0), jnp.where(side.two_valid, b, 0.0)
        return jnp.where(side.even, b, a), jnp.where(side.even, a, b)

    def gather(x, carry):
        rows, slab = rows_of(x * ey, ey), rows_of(x * tall, tall)
        for source, out, (a, b) in (
            (core_in, core_v, (got_one[slab, :], got_two[slab, :])),
            (
                rest_in,
                rest_v,
                [unpack(got.at[main_rows:odd_rows], x, count, tall, halo, LANES - ov - 1, True) for got in (got_one, got_two)],
            ),
        ):
            below, above = sides(a, b)
            value = source[rows, :]
            low, high = value[:tall] + below, value[ey - tall :] + above
            out[rows_of(x * room + ov, ov), :] = jnp.where(side.has_below, low[:ov], 0.0)
            out[rows_of(x * room + tall, ov), :] = low[ov:]
            out[rows_of(x * room + ov + tall, ey - 2 * tall), :] = value[tall : ey - tall]
            out[rows_of(x * room + ov + ey - tall, ov), :] = high[:ov]
            out[rows_of(x * room + ey, ov), :] = jnp.where(side.has_above, high[ov:], 0.0)
        return carry

    lax.fori_loop(0, count, gather, 0, unroll=4)
    for out, start in ((core_v, odd_rows), (rest_v, odd_rows + count)):
        below, above = sides(got_one[start : start + count, :], got_two[start : start + count, :])
        out[pl.ds(ov - 1, count, stride=room), :] = below
        out[pl.ds(ov + ey, count, stride=room), :] = above

    lane = lane_of((ey, RING))
    y = lax.broadcasted_iota(jnp.int32, (ey, RING), 0)
    inside = (lane < cz) | ((lane < cz + ov) & along.has_above) | ((lane >= RING - ov) & along.has_below)
    inside = inside & ((y >= ov) | side.has_below) & ((y < ey - ov) | side.has_above)

    def plane(x):
        at = (info[0] * cx + x) % count
        before, after = jnp.where(at > 0, 1.0, 0.0), jnp.where(at < count - 1, 1.0, 0.0)
        spots = [(x + shift) % count * room + ov for shift in (0, count - 1, 1)]
        halves = []
        for ref in (core_v, rest_v):
            mid, left, right = [ref[rows_of(spot, ey), :] for spot in spots]
            mid_y, left_y, right_y = [ref[pl.ds(spot - 1, ey), :] + ref[pl.ds(spot + 1, ey), :] for spot in spots]
            across, corner = before * left + after * right, before * left_y + after * right_y
            faces = mid_y + across
            halves.append((mid, 0.5 * faces + 0.125 * corner, 0.5 * mid + 0.125 * faces + 0.0625 * corner))
        mid, flat, slope = [jnp.concatenate(pair, axis=1) for pair in zip(*halves)]
        rows = rows_of(x * ey, ey)
        value = block[rows, :] - coef[rows, :] * mid + flat + (pltpu.roll(slope, 1, 1) + pltpu.roll(slope, RING - 1, 1))
        return jnp.where(inside, value, 0.0)

    def store(x, value):
        rows = rows_of(x * ey, ey)
        u[rows, :] = value[:, :LANES]
        far[rows, :] = value[:, LANES:]

    solve(plane, store, (z_on, z_back, y_on, y_back, x_on, x_back, recip), (s0, s1), count, cx, ey, cx)

    def load(x):
        return far[rows_of(x * ey, ey), :]

    pack(load, cx, ey, ov, along.one(0, LANES - ov), one)
    pack(load, cx, ey, ov, along.two(0, LANES - ov), two)

    def keep(x, carry):
        first[rows_of(x * cy, cy), :] = core_v[rows_of(x * room + 2 * ov, cy), :]
        return carry

    lax.fori_loop(0, cx, keep, 0, unroll=8)


def last_sum_z(info, u, got_one, got_two, v, one, two, *, ny, nz, ov, ey, cx, cz):
    side, along = Side(info[1], ny), Side(info[2], nz)

    def add(x, carry):
        rows = rows_of(x * ey, ey)
        value = u[rows, :]
        value = value + unpack(got_one, x, cx, ey, ov, along.one(cz - ov, 0), along.one_valid)
        value = value + unpack(got_two, x, cx, ey, ov, along.two(cz - ov, 0), along.two_valid)
        v[rows, :] = value
        one[rows_of(x * ov, ov), :] = v[rows_of(x * ey + side.one(ey - ov, 0), ov), :]
        two[rows_of(x * ov, ov), :] = v[rows_of(x * ey + side.two(ey - ov, 0), ov), :]
        return carry

    lax.fori_loop(0, cx, add, 0, unroll=8)


def last_sum_y(info, v, got_one, got_two, first, out, *, ny, ov, ey, cx):
    side = Side(info[1], ny)
    cy = ey - 2 * ov

    def add(x, carry):
        a, b = got_one[rows_of(x * ov, ov), :], got_two[rows_of(x * ov, ov), :]
        above, below = jnp.where(side.even, a, b), jnp.where(side.even, b, a)
        above, below = jnp.where(side.has_above, above, 0.0), jnp.where(side.has_below, below, 0.0)
        value = v[rows_of(x * ey + ov, cy), :] + first[rows_of(x * cy, cy), :]
        out[x] = jnp.concatenate([value[:ov] + below, value[ov : cy - ov], value[cy - ov :] + above], axis=0)
        return carry

    lax.fori_loop(0, cx, add, 0, unroll=8)


def make_tables(eigen_x, rest, zt, out, z_on, z_back, *, ov, ez):
    def row(q, carry):
        out[q] = 1.0 / (eigen_x[...] + rest[pl.ds(q, 1), :])
        return carry

    lax.fori_loop(0, out.shape[0], row, 0, unroll=5)

    def fill(table, ref, halo):
        high = table.astype(BF16).astype(F32)
        low = table - high
        ref[:LANES] = high[:LANES].astype(BF16)
        ref[LANES : 2 * LANES] = high[:LANES].astype(BF16)
        ref[2 * LANES : 3 * LANES] = low[:LANES].astype(BF16)
        ref[3 * LANES :] = halo(high, low).astype(BF16)

    def ring(high, low):
        above, below = slice(LANES, LANES + ov), slice(RING - ov, RING)
        parts = [high[above], high[below], high[above], low[below], low[above], jnp.zeros((LANES - 6 * ov, RING), F32), high[below]]
        return jnp.concatenate(parts, axis=0)

    def plain(high, low):
        tail = slice(LANES, ez)
        parts = [high[tail], high[tail], low[tail], jnp.zeros((LANES - 3 * (ez - LANES), RING), F32)]
        return jnp.concatenate(parts, axis=0)

    table = zt[...]
    fill(table, z_on, ring)
    fill(table.T, z_back, plain)


def gather_x(block):
    count = lax.axis_size("gx")
    parts = [block]
    for shift in range(1, count):
        parts.append(lax.ppermute(block, "gx", [((i + shift) % count, i) for i in range(count)]))
    return parts


def columns(table):
    high = lax.reduce_precision(table, 8, 7)
    return jnp.concatenate([high, table - high, high], axis=1).astype(BF16)


def local(right_side, reaction, basis_x, basis_y, basis_z, eigen_x, eigen_y, eigen_z):
    cx, cy, cz = right_side.shape
    ex, ey, ez = basis_x.shape[0], basis_y.shape[0], basis_z.shape[0]
    ov = (ex - cx) // 2
    nx, ny, nz = lax.axis_size("gx"), lax.axis_size("gy"), lax.axis_size("gz")
    ix, iy, iz = lax.axis_index("gx"), lax.axis_index("gy"), lax.axis_index("gz")
    count = nx * cx
    info = jnp.stack([ix, iy, iz]).astype(jnp.int32)
    w, tall, halo = 2 * ov + 1, 2 * ov, 2 * (ov + 1)
    at = dict(ov=ov, ey=ey, cz=cz)

    f_parts = gather_x(right_side)

    blocks = [jnp.pad(basis_x.T, ((0, 0), (i * cx, (nx - 1 - i) * cx)))[:, ov : ov + count] for i in range(nx)]
    table = jnp.concatenate(blocks, axis=0)
    table = lax.dynamic_slice_in_dim(jnp.concatenate([table, table], axis=1), ix * cx, count, axis=1)
    zero = jnp.zeros((ey, ey), F32)
    double = jnp.concatenate([jnp.concatenate([basis_y, zero], axis=1), jnp.concatenate([zero, basis_y], axis=1)], axis=0)
    zt = jnp.concatenate([basis_z[ov:], jnp.zeros((RING - ez, ez), F32), basis_z[:ov]], axis=0)
    zt = jnp.pad(zt, ((0, 0), (0, RING - ez)))
    rest = eigen_y[:, None] + eigen_z[None, :]
    rest = jnp.concatenate([rest[:, :LANES], rest[:, LANES:].reshape(-1, LANES)], axis=0)
    recip, z_on, z_back = call(
        functools.partial(make_tables, ov=ov, ez=ez), [(rest.shape[0], ex, LANES), (4 * LANES, RING, BF16), (4 * LANES, RING, BF16)],
        jnp.broadcast_to(eigen_x[:, None], (ex, LANES)), rest, zt, smem=0,
    )
    tables = (z_on, z_back, columns(double.T), columns(double), columns(table), columns(table.T), recip)

    slabs = call(functools.partial(first_slabs, ny=ny, ov=ov), [(count + cx, ov, cz)] * 2, info, *f_parts, reaction)
    got = swap(*slabs, "gy")
    edge = group_of(cx, ov) * ey
    small = (group_of(count, ov) * ey + edge, LANES)
    f, c, *slabs = call(
        functools.partial(second_slabs, ny=ny, nz=nz, ov=ov), [(count * ey, cz), (cx * ey, cz), small, small], info, *f_parts, reaction, *got
    )
    got = swap(*slabs, "gz")
    c_parts = gather_x(c)
    state = [pltpu.VMEM((count * ey, LANES), F32), pltpu.VMEM((ey // 8 * count, LANES), F32)]
    small = (group_of(count, w) * ey, LANES)
    u, block, rest, *slabs = call(
        functools.partial(first_solve, nz=nz, cx=cx, **at), [(count * ey, RING)] * 2 + [(2 * edge, LANES), small, small], info, f, *got, *tables, scratch=state
    )
    got = swap(*slabs, "gz")
    c_parts += gather_x(rest)
    tall_rows = (count * tall + group_of(count, halo) * tall + 2 * count, LANES)
    core, rest, *slabs = call(functools.partial(sum_z, ny=ny, nz=nz, **at), [(count * ey, LANES)] * 2 + [tall_rows, tall_rows], info, u, *got)
    got = swap(*slabs, "gy")
    c = call(functools.partial(coefficients, nz=nz, ov=ov, ey=ey), [(count * ey, RING)], info, *c_parts, after=slabs[:1])[0]
    small = (group_of(cx, ov) * ey, LANES)
    state += [pltpu.VMEM((count * (ey + 2 * ov), LANES), F32)] * 2 + [pltpu.VMEM((cx * ey, LANES), F32)]
    u, first, *slabs = call(
        functools.partial(second_solve, ny=ny, nz=nz, cx=cx, **at),
        [(cx * ey, LANES), (cx * cy, LANES), small, small], info, core, rest, *got, block, c, *tables, scratch=state,
    )
    got = swap(*slabs, "gz")
    v, *slabs = call(functools.partial(last_sum_z, ny=ny, nz=nz, cx=cx, **at), [(cx * ey, LANES)] + [(cx * ov, LANES)] * 2, info, u, *got)
    got = swap(*slabs, "gy")
    return call(functools.partial(last_sum_y, ny=ny, ov=ov, ey=ey, cx=cx), [(cx, cy, cz)], info, v, *got, first)[0]


def solution(mesh):
    return jax.shard_map(
        local,
        mesh=mesh,
        in_specs=(P("gx", "gy", "gz"), P("gx", "gy", "gz"), P(), P(), P(), P(), P(), P()),
        out_specs=P("gx", "gy", "gz"),
        check_vma=False,
    )
```

```python
import functools
import math

import jax
import jax.numpy as jnp
from jax import lax
from jax.experimental import pallas as pl
from jax.experimental.pallas import tpu as pltpu
from jax.sharding import PartitionSpec as P


LANES = 128
RING = 256
F32 = jnp.float32
BF16 = jnp.bfloat16


def pairs(count, first, around):
    swaps = {}
    for low in range(first, count - 1, 2):
        swaps[low], swaps[low + 1] = low + 1, low
    if around and first == 1 and count % 2 == 0 and count > 2:
        swaps[0], swaps[count - 1] = count - 1, 0
    return [(i, swaps.get(i, i)) for i in range(count)]


def swap(one, two, axis, around=False):
    count = lax.axis_size(axis)
    return lax.ppermute(one, axis, pairs(count, 0, around)), lax.ppermute(two, axis, pairs(count, 1, around))


def call(kernel, outs, *args, scratch=(), smem=1, after=()):
    vmem = pl.BlockSpec(memory_space=pltpu.VMEM)
    specs = [pl.BlockSpec(memory_space=pltpu.SMEM)] * smem + [vmem] * (len(args) - smem)
    specs += [pl.BlockSpec(memory_space=pl.ANY)] * len(after)
    used = len(args)
    held = sum(math.prod(s.shape) * 4 for s in scratch)

    def body(*refs):
        kernel(*refs[:used], *refs[used + len(after) :])

    return pl.pallas_call(
        body,
        out_shape=[jax.ShapeDtypeStruct(s[:2], BF16) if BF16 in s else jax.ShapeDtypeStruct(s, F32) for s in outs],
        in_specs=specs,
        out_specs=[vmem] * len(outs),
        scratch_shapes=list(scratch),
        compiler_params=pltpu.CompilerParams(vmem_limit_bytes=held + 6 * 1024 * 1024),
    )(*args, *after)


class Side:
    def __init__(self, index, count):
        self.even = index % 2 == 0
        self.has_below = index > 0
        self.has_above = index < count - 1
        self.one_valid = jnp.where(self.even, self.has_above, self.has_below)
        self.two_valid = jnp.where(self.even, self.has_below, self.has_above)

    def one(self, above, below):
        return jnp.where(self.even, above, below)

    def two(self, above, below):
        return jnp.where(self.even, below, above)


def rows_of(start, size):
    return pl.ds(pl.multiple_of(start, 8), size)


def lane_of(shape):
    return lax.broadcasted_iota(jnp.int32, shape, 1)


def group_of(count, width):
    return -(-count // (LANES // width))


def odd_group(count, width):
    return next(n for n in range(8, count + 1, 8) if count % n == 0 and count // n * width <= LANES)


def pack(load, count, rows, width, src, out):
    each = group_of(count, width)
    lane = lane_of((rows, LANES))

    def member(j, carry):
        value = jnp.zeros((rows, LANES), F32)
        for g in range(-(-count // each)):
            x = jnp.minimum(g * each + j, count - 1)
            turned = pltpu.roll(load(x), (g * width - src + LANES) % LANES, 1)
            value = jnp.where((lane >= g * width) & (lane < (g + 1) * width), turned, value)
        out[rows_of(j * rows, rows), :] = value
        return carry

    lax.fori_loop(0, each, member, 0, unroll=min(each, 8))


def unpack(ref, x, count, rows, width, dst, valid):
    each = group_of(count, width)
    g, j = x // each, x % each
    turned = pltpu.roll(ref[rows_of(j * rows, rows), :], (dst - g * width + LANES) % LANES, 1)
    away = (lane_of((rows, LANES)) - dst + LANES) % LANES
    return jnp.where((away < width) & valid, turned, 0.0)


def split(value):
    high = value.astype(BF16)
    return high, (value - high.astype(F32)).astype(BF16)


def stack_rows(value):
    high, low = split(value)
    return jnp.concatenate([high, high, low], axis=0)


def dot(a, b):
    return jnp.dot(a, b, preferred_element_type=F32)


def first_slabs(info, *refs, ny, ov):
    parts, (one, two) = refs[:-2], refs[-2:]
    side = Side(info[1], ny)
    cx, cy, _ = parts[0].shape
    for k, part in enumerate(parts):
        one[k * cx : (k + 1) * cx] = part[:, rows_of(side.one(cy - ov, 0), ov), :]
        two[k * cx : (k + 1) * cx] = part[:, rows_of(side.two(cy - ov, 0), ov), :]


def second_slabs(info, *refs, ny, nz, ov):
    parts, (got_one, got_two, field, coef, one, two) = refs[:-6], refs[-6:]
    side, along = Side(info[1], ny), Side(info[2], nz)
    cx, cy, cz = parts[0].shape
    ey = cy + 2 * ov
    count = (len(parts) - 1) * cx
    for k, part in enumerate(parts):
        out, first = (coef, 0) if k == len(parts) - 1 else (field, k * cx)

        def place(x, carry, k=k, part=part, out=out, first=first):
            a = got_one[k * cx + x]
            b = got_two[k * cx + x]
            row = (first + x) * ey
            above = jnp.where(side.even, a, b)
            below = jnp.where(side.even, b, a)
            out[rows_of(row, ov), :] = jnp.where(side.has_below, below, 0.0)
            out[rows_of(row + ov, cy), :] = part[x]
            out[rows_of(row + ov + cy, ov), :] = jnp.where(side.has_above, above, 0.0)
            return carry

        lax.fori_loop(0, cx, place, 0, unroll=24)

    edge = group_of(count, ov) * ey
    for ref, planes, first in ((field, count, 0), (coef, cx, edge)):

        def load(x, ref=ref):
            return ref[rows_of(x * ey, ey), :]

        last = first + group_of(planes, ov) * ey
        pack(load, planes, ey, ov, along.one(cz - ov, 0), one.at[first:last])
        pack(load, planes, ey, ov, along.two(cz - ov, 0), two.at[first:last])


def extended(field, got_one, got_two, x, count, ey, ov, along):
    halo = unpack(got_one, x, count, ey, ov, along.one(0, LANES - ov), along.one_valid)
    halo = halo + unpack(got_two, x, count, ey, ov, along.two(0, LANES - ov), along.two_valid)
    return jnp.concatenate([field[rows_of(x * ey, ey), :], halo], axis=1)


def turn(value):
    group = LANES // 8
    row = lax.broadcasted_iota(jnp.int32, (8, LANES), 0)
    column = lane_of((8, LANES)) // group
    for bit in (4, 2, 1):
        up = pltpu.roll(pltpu.roll(value, 8 - bit, 0), bit * group, 1)
        down = pltpu.roll(pltpu.roll(value, bit, 0), LANES - bit * group, 1)
        moved = jnp.where((row & bit) == 0, up, down)
        value = jnp.where((row & bit) == (column & bit), value, moved)
    return value


def solve(source, store, tables, state, count, back, ey, cx):
    z_on, z_back, y_on, y_back, x_on, x_back, recip = tables
    s0, s1 = state
    modes = recip.shape[1]
    group = LANES // 8
    lane = lane_of((ey, LANES))
    octs = ey // 8
    nothing = jnp.zeros((ey, LANES), F32)

    def times_y(table, core, sides):
        planes = [core[j * ey : (j + 1) * ey] for j in range(cx)] + sides
        planes += [nothing] * (-len(planes) % 4)
        done = []
        for j in range(0, len(planes), 4):
            quad = jnp.concatenate([jnp.concatenate(planes[j + i : j + i + 2], axis=0) for i in (0, 2)], axis=1)
            quad = dot(table[...], stack_rows(quad))
            done += [quad[i * ey : (i + 1) * ey, k * LANES : (k + 1) * LANES] for k in range(2) for i in range(2)]
        return done[:cx], done[cx : cx + len(sides)]

    def on(part, carry):
        rows = []
        for j in range(cx):
            value = source(part * cx + j)
            high, low = split(value[:, :LANES])
            near = value[:, LANES:].astype(BF16).astype(F32)
            halo = near + pltpu.roll(value[:, LANES:] - near, group, 1) + pltpu.roll(near, 2 * group, 1)
            rows.append((high, low, high, halo.astype(BF16)))
        value = dot(jnp.concatenate([jnp.concatenate(piece, axis=0) for piece in zip(*rows)], axis=1), z_on[...])
        sides = []
        for k in range(cx // 8):
            side = nothing
            for j in range(8):
                turned = pltpu.roll(value[(8 * k + j) * ey : (8 * k + j + 1) * ey, LANES:], j * group, 1)
                side = jnp.where(lane // group == j, turned, side)
            sides.append(side)
        core, sides = times_y(y_on, value[:, :LANES], sides)
        for j in range(cx):
            s0[rows_of((part * cx + j) * ey, ey), :] = core[j]
        for k in range(cx // 8):
            for q in range(octs):
                s1[rows_of(q * count + part * cx + k * 8, 8), :] = turn(sides[k][q * 8 : (q + 1) * 8])
        return carry

    lax.fori_loop(0, count // cx, on, 0, unroll=2)

    def times_x(value, factor):
        value = dot(x_on[...], stack_rows(value))
        value = jnp.concatenate([value[i * modes : (i + 1) * modes] * factor for i in range(value.shape[0] // modes)], axis=0)
        return dot(x_back[...], stack_rows(value))[:back]

    def middle(h, carry):
        q = 2 * h
        value = [s0[pl.ds(q + i, count, stride=ey), :] for i in range(2)]
        value = times_x(jnp.concatenate(value, axis=1), jnp.concatenate([recip[q], recip[q + 1]], axis=1))
        for i in range(2):
            s0[pl.ds(q + i, back, stride=ey), :] = value[:, i * LANES : (i + 1) * LANES]
        return carry

    for q in range(octs):
        value = times_x(s1[q * count : (q + 1) * count, :], recip[ey + q])
        s1[q * count : q * count + back, :] = value
    lax.fori_loop(0, ey // 2, middle, 0, unroll=20)

    def off(part, carry):
        sides = []
        for k in range(cx // 8):
            sides.append(jnp.concatenate([turn(s1[rows_of(q * count + part * cx + k * 8, 8), :]) for q in range(octs)], axis=0))
        core, sides = times_y(y_back, s0[rows_of(part * cx * ey, cx * ey), :], sides)
        rows = []
        for k in range(cx // 8):
            near = sides[k].astype(BF16).astype(F32)
            far = sides[k] - near
            for j in range(8):
                high, low = split(core[8 * k + j])
                halo = [pltpu.roll(piece, (i - j) * group % LANES, 1) for i, piece in enumerate((near, far, near))]
                halo = jnp.where(lane < group, halo[0], jnp.where(lane < 2 * group, halo[1], halo[2]))
                rows.append((high, low, high, halo.astype(BF16)))
        value = dot(jnp.concatenate([jnp.concatenate(piece, axis=0) for piece in zip(*rows)], axis=1), z_back[...])
        for j in range(cx):
            store(part * cx + j, value[j * ey : (j + 1) * ey])
        return carry

    lax.fori_loop(0, back // cx, off, 0, unroll=2 if back > cx else 1)


def merged(core, halo, low):
    lane = lane_of(core.shape)
    return jnp.where((lane < LANES // 2) == low, core, halo)


def first_solve(info, field, got_one, got_two, z_on, z_back, y_on, y_back, x_on, x_back, recip, u, block, rest, one, two, s0, s1, *, nz, ov, ey, cx, cz):
    along = Side(info[2], nz)
    count = field.shape[0] // ey
    w = 2 * ov + 1
    edge, half = group_of(count, ov) * ey, rest.shape[0] // 2
    rest[:half] = got_one[edge:]
    rest[half:] = got_two[edge:]

    def source(x):
        value = extended(field, got_one, got_two, x, count, ey, ov, along)
        block[rows_of(x * ey, ey), :] = value
        return value

    def store(x, value):
        u[rows_of(x * ey, ey), :] = value

    solve(source, store, (z_on, z_back, y_on, y_back, x_on, x_back, recip), (s0, s1), count, count, ey, cx)

    for out, low in ((one, ~along.even), (two, along.even)):

        def load(x, low=low):
            rows = rows_of(x * ey, ey)
            return merged(u[rows, :LANES], u[rows, LANES:], low)

        pack(load, count, ey, w, jnp.where(low, LANES - ov, cz - ov - 1), out)


def sum_z(info, u, got_one, got_two, core_out, rest_out, one, two, *, ny, nz, ov, ey, cz):
    side, along = Side(info[1], ny), Side(info[2], nz)
    count = u.shape[0] // ey
    w = 2 * ov + 1
    lane = lane_of((ey, LANES))
    inside = ((lane <= ov) & along.has_above) | ((lane >= LANES - ov - 1) & along.has_below)

    def add(x, carry):
        rows = rows_of(x * ey, ey)
        core, rest = u[rows, :LANES], u[rows, LANES:]
        for got, low, valid in ((got_one, ~along.even, along.one_valid), (got_two, along.even, along.two_valid)):
            part = unpack(got, x, count, ey, w, jnp.where(low, LANES - ov - 1, cz - ov), valid)
            mine = (lane < LANES // 2) == low
            core, rest = core + jnp.where(mine, part, 0.0), rest + jnp.where(mine, 0.0, part)
        core_out[rows, :] = core
        rest_out[rows, :] = jnp.where(inside, rest, 0.0)
        return carry

    lax.fori_loop(0, count, add, 0, unroll=16)
    tall, halo = 2 * ov, 2 * (ov + 1)
    wide = group_of(count, halo)
    for out, high in ((one, side.even), (two, ~side.even)):
        start = jnp.where(high, ey - tall, 0)
        odd = pl.ds(jnp.where(high, ey - tall - 1, tall), count, stride=ey)

        def main(x, carry, out=out, start=start):
            out[rows_of(x * tall, tall), :] = core_out[rows_of(x * ey + start, tall), :]
            return carry

        lax.fori_loop(0, count, main, 0, unroll=16)
        base = count * tall

        def load(x, start=start):
            return rest_out[rows_of(x * ey + start, tall), :]

        pack(load, count, tall, halo, LANES - ov - 1, out.at[base : base + wide * tall])
        base = base + wide * tall
        out[base : base + count, :] = core_out[odd, :]
        rows = rest_out[odd, :]
        each = odd_group(count, halo)
        near = lane_of((each, LANES))
        value = jnp.zeros((each, LANES), F32)
        for g in range(count // each):
            turned = pltpu.roll(rows[g * each : (g + 1) * each], (g * halo + ov + 1) % LANES, 1)
            value = jnp.where((near >= g * halo) & (near < (g + 1) * halo), turned, value)
        out[base + count :, :] = value


def coefficients(info, *refs, nz, ov, ey):
    parts, out = refs[:-1], refs[-1]
    along = Side(info[2], nz)
    half = len(parts) // 2
    cx = parts[0].shape[0] // ey
    for k in range(half):
        core, rest = parts[k], parts[half + k]
        edge = rest.shape[0] // 2

        def plane(x, carry, k=k, core=core, rest=rest, edge=edge):
            value = extended(core, rest.at[:edge], rest.at[edge:], x, cx, ey, ov, along)
            out[rows_of((k * cx + x) * ey, ey), :] = value + 5.0
            return carry

        lax.fori_loop(0, cx, plane, 0, unroll=4)


def second_solve(info, core_in, rest_in, got_one, got_two, block, coef, z_on, z_back, y_on, y_back, x_on, x_back, recip, u, first, one, two, s0, s1, core_v, rest_v, far, *, ny, nz, ov, ey, cx, cz):
    side, along = Side(info[1], ny), Side(info[2], nz)
    count = coef.shape[0] // ey
    tall, halo = 2 * ov, 2 * (ov + 1)
    each = group_of(count, halo)
    room = ey + 2 * ov
    cy = ey - 2 * ov
    main_rows = count * tall
    odd_rows = main_rows + each * tall

    def sides(a, b):
        a, b = jnp.where(side.one_valid, a, 0.0), jnp.where(side.two_valid, b, 0.0)
        return jnp.where(side.even, b, a), jnp.where(side.even, a, b)

    def gather(x, carry):
        rows, slab = rows_of(x * ey, ey), rows_of(x * tall, tall)
        for source, out, (a, b) in (
            (core_in, core_v, (got_one[slab, :], got_two[slab, :])),
            (
                rest_in,
                rest_v,
                [unpack(got.at[main_rows:odd_rows], x, count, tall, halo, LANES - ov - 1, True) for got in (got_one, got_two)],
            ),
        ):
            below, above = sides(a, b)
            value = source[rows, :]
            low, high = value[:tall] + below, value[ey - tall :] + above
            out[rows_of(x * room + ov, ov), :] = jnp.where(side.has_below, low[:ov], 0.0)
            out[rows_of(x * room + tall, ov), :] = low[ov:]
            out[rows_of(x * room + ov + tall, ey - 2 * tall), :] = value[tall : ey - tall]
            out[rows_of(x * room + ov + ey - tall, ov), :] = high[:ov]
            out[rows_of(x * room + ey, ov), :] = jnp.where(side.has_above, high[ov:], 0.0)
        return carry

    lax.fori_loop(0, count, gather, 0, unroll=8)
    single = odd_group(count, halo)
    near = lane_of((single, LANES))

    def odd(ref):
        value = ref[odd_rows + count :, :]
        rows = [pltpu.roll(value, (2 * LANES - g * halo - ov - 1) % LANES, 1) for g in range(count // single)]
        return jnp.concatenate([jnp.where((near <= ov) | (near >= LANES - ov - 1), row, 0.0) for row in rows], axis=0)

    for out, a, b in (
        (core_v, got_one[odd_rows : odd_rows + count, :], got_two[odd_rows : odd_rows + count, :]),
        (rest_v, odd(got_one), odd(got_two)),
    ):
        below, above = sides(a, b)
        out[pl.ds(ov - 1, count, stride=room), :] = below
        out[pl.ds(ov + ey, count, stride=room), :] = above

    lane = lane_of((ey, RING))
    y = lax.broadcasted_iota(jnp.int32, (ey, RING), 0)
    inside = (lane < cz) | ((lane < cz + ov) & along.has_above) | ((lane >= RING - ov) & along.has_below)
    inside = inside & ((y >= ov) | side.has_below) & ((y < ey - ov) | side.has_above)

    def plane(x):
        at = (info[0] * cx + x) % count
        before, after = jnp.where(at > 0, 1.0, 0.0), jnp.where(at < count - 1, 1.0, 0.0)
        spots = [(x + shift) % count * room + ov for shift in (0, count - 1, 1)]
        halves = []
        for ref in (core_v, rest_v):
            mid, left, right = [ref[rows_of(spot, ey), :] for spot in spots]
            mid_y, left_y, right_y = [ref[pl.ds(spot - 1, ey), :] + ref[pl.ds(spot + 1, ey), :] for spot in spots]
            across, corner = before * left + after * right, before * left_y + after * right_y
            faces = mid_y + across
            halves.append((mid, 0.5 * faces + 0.125 * corner, 0.5 * mid + 0.125 * faces + 0.0625 * corner))
        mid, flat, slope = [jnp.concatenate(pair, axis=1) for pair in zip(*halves)]
        rows = rows_of(x * ey, ey)
        value = block[rows, :] - coef[rows, :] * mid + flat + (pltpu.roll(slope, 1, 1) + pltpu.roll(slope, RING - 1, 1))
        return jnp.where(inside, value, 0.0)

    def store(x, value):
        rows = rows_of(x * ey, ey)
        u[rows, :] = value[:, :LANES]
        far[rows, :] = value[:, LANES:]

    solve(plane, store, (z_on, z_back, y_on, y_back, x_on, x_back, recip), (s0, s1), count, cx, ey, cx)

    def load(x):
        return far[rows_of(x * ey, ey), :]

    pack(load, cx, ey, ov, along.one(0, LANES - ov), one)
    pack(load, cx, ey, ov, along.two(0, LANES - ov), two)

    def keep(x, carry):
        first[rows_of(x * cy, cy), :] = core_v[rows_of(x * room + 2 * ov, cy), :]
        return carry

    lax.fori_loop(0, cx, keep, 0, unroll=8)


def last_sum_z(info, u, got_one, got_two, v, one, two, *, ny, nz, ov, ey, cx, cz):
    side, along = Side(info[1], ny), Side(info[2], nz)

    def add(x, carry):
        rows = rows_of(x * ey, ey)
        value = u[rows, :]
        value = value + unpack(got_one, x, cx, ey, ov, along.one(cz - ov, 0), along.one_valid)
        value = value + unpack(got_two, x, cx, ey, ov, along.two(cz - ov, 0), along.two_valid)
        v[rows, :] = value
        one[rows_of(x * ov, ov), :] = v[rows_of(x * ey + side.one(ey - ov, 0), ov), :]
        two[rows_of(x * ov, ov), :] = v[rows_of(x * ey + side.two(ey - ov, 0), ov), :]
        return carry

    lax.fori_loop(0, cx, add, 0, unroll=24)


def last_sum_y(info, v, got_one, got_two, first, out, *, ny, ov, ey, cx):
    side = Side(info[1], ny)
    cy = ey - 2 * ov

    def add(x, carry):
        a, b = got_one[rows_of(x * ov, ov), :], got_two[rows_of(x * ov, ov), :]
        above, below = jnp.where(side.even, a, b), jnp.where(side.even, b, a)
        above, below = jnp.where(side.has_above, above, 0.0), jnp.where(side.has_below, below, 0.0)
        value = v[rows_of(x * ey + ov, cy), :] + first[rows_of(x * cy, cy), :]
        out[x] = jnp.concatenate([value[:ov] + below, value[ov : cy - ov], value[cy - ov :] + above], axis=0)
        return carry

    lax.fori_loop(0, cx, add, 0, unroll=24)


def make_tables(eigen_x, rest, zt, out, z_on, z_back, *, ov, ez):
    def row(q, carry):
        out[q] = 1.0 / (eigen_x[...] + rest[pl.ds(q, 1), :])
        return carry

    lax.fori_loop(0, out.shape[0], row, 0, unroll=5)

    def fill(table, ref, halo):
        high = table.astype(BF16).astype(F32)
        low = table - high
        ref[:LANES] = high[:LANES].astype(BF16)
        ref[LANES : 2 * LANES] = high[:LANES].astype(BF16)
        ref[2 * LANES : 3 * LANES] = low[:LANES].astype(BF16)
        ref[3 * LANES :] = halo(high, low).astype(BF16)

    def ring(high, low):
        above, below = slice(LANES, LANES + ov), slice(RING - ov, RING)
        parts = [high[above], high[below], high[above], low[below], low[above], jnp.zeros((LANES - 6 * ov, RING), F32), high[below]]
        return jnp.concatenate(parts, axis=0)

    def plain(high, low):
        tail = slice(LANES, ez)
        parts = [high[tail], high[tail], low[tail], jnp.zeros((LANES - 3 * (ez - LANES), RING), F32)]
        return jnp.concatenate(parts, axis=0)

    table = zt[...]
    fill(table, z_on, ring)
    fill(table.T, z_back, plain)


def gather_x(block):
    count = lax.axis_size("gx")
    parts = [block]
    for shift in range(1, count):
        parts.append(lax.ppermute(block, "gx", [((i + shift) % count, i) for i in range(count)]))
    return parts


def columns(table):
    high = lax.reduce_precision(table, 8, 7)
    return jnp.concatenate([high, table - high, high], axis=1).astype(BF16)


def local(right_side, reaction, basis_x, basis_y, basis_z, eigen_x, eigen_y, eigen_z):
    cx, cy, cz = right_side.shape
    ex, ey, ez = basis_x.shape[0], basis_y.shape[0], basis_z.shape[0]
    ov = (ex - cx) // 2
    nx, ny, nz = lax.axis_size("gx"), lax.axis_size("gy"), lax.axis_size("gz")
    ix, iy, iz = lax.axis_index("gx"), lax.axis_index("gy"), lax.axis_index("gz")
    count = nx * cx
    info = jnp.stack([ix, iy, iz]).astype(jnp.int32)
    w, tall, halo = 2 * ov + 1, 2 * ov, 2 * (ov + 1)
    at = dict(ov=ov, ey=ey, cz=cz)

    f_parts = gather_x(right_side)

    blocks = [jnp.pad(basis_x.T, ((0, 0), (i * cx, (nx - 1 - i) * cx)))[:, ov : ov + count] for i in range(nx)]
    table = jnp.concatenate(blocks, axis=0)
    table = lax.dynamic_slice_in_dim(jnp.concatenate([table, table], axis=1), ix * cx, count, axis=1)
    zero = jnp.zeros((ey, ey), F32)
    double = jnp.concatenate([jnp.concatenate([basis_y, zero], axis=1), jnp.concatenate([zero, basis_y], axis=1)], axis=0)
    zt = jnp.concatenate([basis_z[ov:], jnp.zeros((RING - ez, ez), F32), basis_z[:ov]], axis=0)
    zt = jnp.pad(zt, ((0, 0), (0, RING - ez)))
    rest = eigen_y[:, None] + eigen_z[None, :]
    rest = jnp.concatenate([rest[:, :LANES], rest[:, LANES:].reshape(-1, LANES)], axis=0)
    recip, z_on, z_back = call(
        functools.partial(make_tables, ov=ov, ez=ez), [(rest.shape[0], ex, LANES), (4 * LANES, RING, BF16), (4 * LANES, RING, BF16)],
        jnp.broadcast_to(eigen_x[:, None], (ex, LANES)), rest, zt, smem=0,
    )
    tables = (z_on, z_back, columns(double.T), columns(double), columns(table), columns(table.T), recip)

    slabs = call(functools.partial(first_slabs, ny=ny, ov=ov), [(count + cx, ov, cz)] * 2, info, *f_parts, reaction)
    got = swap(*slabs, "gy")
    edge = group_of(cx, ov) * ey
    small = (group_of(count, ov) * ey + edge, LANES)
    f, c, *slabs = call(
        functools.partial(second_slabs, ny=ny, nz=nz, ov=ov), [(count * ey, cz), (cx * ey, cz), small, small], info, *f_parts, reaction, *got
    )
    got = swap(*slabs, "gz", around=True)
    c_parts = gather_x(c)
    state = [pltpu.VMEM((count * ey, LANES), F32), pltpu.VMEM((ey // 8 * count, LANES), F32)]
    small = (group_of(count, w) * ey, LANES)
    u, block, rest, *slabs = call(
        functools.partial(first_solve, nz=nz, cx=cx, **at), [(count * ey, RING)] * 2 + [(2 * edge, LANES), small, small], info, f, *got, *tables, scratch=state
    )
    got = swap(*slabs, "gz")
    c_parts += gather_x(rest)
    tall_rows = (count * tall + group_of(count, halo) * tall + count + odd_group(count, halo), LANES)
    core, rest, *slabs = call(functools.partial(sum_z, ny=ny, nz=nz, **at), [(count * ey, LANES)] * 2 + [tall_rows, tall_rows], info, u, *got)
    got = swap(*slabs, "gy")
    c = call(functools.partial(coefficients, nz=nz, ov=ov, ey=ey), [(count * ey, RING)], info, *c_parts, after=slabs[:1])[0]
    small = (group_of(cx, ov) * ey, LANES)
    state += [pltpu.VMEM((count * (ey + 2 * ov), LANES), F32)] * 2 + [pltpu.VMEM((cx * ey, LANES), F32)]
    u, first, *slabs = call(
        functools.partial(second_solve, ny=ny, nz=nz, cx=cx, **at),
        [(cx * ey, LANES), (cx * cy, LANES), small, small], info, core, rest, *got, block, c, *tables, scratch=state,
    )
    got = swap(*slabs, "gz", around=True)
    v, *slabs = call(functools.partial(last_sum_z, ny=ny, nz=nz, cx=cx, **at), [(cx * ey, LANES)] + [(cx * ov, LANES)] * 2, info, u, *got)
    got = swap(*slabs, "gy")
    return call(functools.partial(last_sum_y, ny=ny, ov=ov, ey=ey, cx=cx), [(cx, cy, cz)], info, v, *got, first)[0]


def solution(mesh):
    return jax.shard_map(
        local,
        mesh=mesh,
        in_specs=(P("gx", "gy", "gz"), P("gx", "gy", "gz"), P(), P(), P(), P(), P(), P()),
        out_specs=P("gx", "gy", "gz"),
        check_vma=False,
    )
```

```python
import functools
import math

import jax
import jax.numpy as jnp
from jax import lax
from jax.experimental import pallas as pl
from jax.experimental.pallas import tpu as pltpu
from jax.sharding import PartitionSpec as P


LANES = 128
RING = 256
F32 = jnp.float32
BF16 = jnp.bfloat16


def pairs(count, first, around):
    swaps = {}
    for low in range(first, count - 1, 2):
        swaps[low], swaps[low + 1] = low + 1, low
    if around and first == 1 and count % 2 == 0 and count > 2:
        swaps[0], swaps[count - 1] = count - 1, 0
    return [(i, swaps.get(i, i)) for i in range(count)]


def swap(one, two, axis, around=False):
    count = lax.axis_size(axis)
    return lax.ppermute(one, axis, pairs(count, 0, around)), lax.ppermute(two, axis, pairs(count, 1, around))


class Place:
    def __getitem__(self, axis):
        return lax.axis_index(("gx", "gy", "gz")[axis])


def call(kernel, outs, *args, scratch=(), after=()):
    vmem = pl.BlockSpec(memory_space=pltpu.VMEM)
    specs = [vmem] * len(args) + [pl.BlockSpec(memory_space=pl.ANY)] * len(after)
    used = len(args)
    held = sum(math.prod(s.shape) * 4 for s in scratch)

    def body(*refs):
        kernel(Place(), *refs[:used], *refs[used + len(after) :])

    return pl.pallas_call(
        body,
        out_shape=[jax.ShapeDtypeStruct(s[:2], BF16) if BF16 in s else jax.ShapeDtypeStruct(s, F32) for s in outs],
        in_specs=specs,
        out_specs=[vmem] * len(outs),
        scratch_shapes=list(scratch),
        compiler_params=pltpu.CompilerParams(vmem_limit_bytes=held + 6 * 1024 * 1024),
    )(*args, *after)


class Side:
    def __init__(self, index, count):
        self.even = index % 2 == 0
        self.has_below = index > 0
        self.has_above = index < count - 1
        self.one_valid = jnp.where(self.even, self.has_above, self.has_below)
        self.two_valid = jnp.where(self.even, self.has_below, self.has_above)

    def one(self, above, below):
        return jnp.where(self.even, above, below)

    def two(self, above, below):
        return jnp.where(self.even, below, above)


def rows_of(start, size):
    return pl.ds(pl.multiple_of(start, 8), size)


def lane_of(shape):
    return lax.broadcasted_iota(jnp.int32, shape, 1)


def group_of(count, width):
    return -(-count // (LANES // width))


def odd_group(count, width):
    return next(n for n in range(8, count + 1, 8) if count % n == 0 and count // n * width <= LANES)


def pack(load, count, rows, width, src, out):
    each = group_of(count, width)
    lane = lane_of((rows, LANES))

    def member(j, carry):
        value = jnp.zeros((rows, LANES), F32)
        for g in range(-(-count // each)):
            x = jnp.minimum(g * each + j, count - 1)
            turned = pltpu.roll(load(x), (g * width - src + LANES) % LANES, 1)
            value = jnp.where((lane >= g * width) & (lane < (g + 1) * width), turned, value)
        out[rows_of(j * rows, rows), :] = value
        return carry

    lax.fori_loop(0, each, member, 0, unroll=min(each, 8))


def unpack(ref, x, count, rows, width, dst, valid):
    each = group_of(count, width)
    g, j = x // each, x % each
    turned = pltpu.roll(ref[rows_of(j * rows, rows), :], (dst - g * width + LANES) % LANES, 1)
    away = (lane_of((rows, LANES)) - dst + LANES) % LANES
    return jnp.where((away < width) & valid, turned, 0.0)


def split(value):
    high = value.astype(BF16)
    return high, (value - high.astype(F32)).astype(BF16)


def stack_rows(value):
    high, low = split(value)
    return jnp.concatenate([high, high, low], axis=0)


def dot(a, b):
    return jnp.dot(a, b, preferred_element_type=F32)


def first_slabs(info, *refs, ny, ov):
    parts, (one, two) = refs[:-2], refs[-2:]
    side = Side(info[1], ny)
    cx, cy, _ = parts[0].shape
    for k, part in enumerate(parts):
        one[k * cx : (k + 1) * cx] = part[:, rows_of(side.one(cy - ov, 0), ov), :]
        two[k * cx : (k + 1) * cx] = part[:, rows_of(side.two(cy - ov, 0), ov), :]


def second_slabs(info, *refs, ny, nz, ov):
    parts, (got_one, got_two, field, coef, one, two) = refs[:-6], refs[-6:]
    side, along = Side(info[1], ny), Side(info[2], nz)
    cx, cy, cz = parts[0].shape
    ey = cy + 2 * ov
    count = (len(parts) - 1) * cx
    for k, part in enumerate(parts):
        out, first = (coef, 0) if k == len(parts) - 1 else (field, k * cx)

        def place(x, carry, k=k, part=part, out=out, first=first):
            a = got_one[k * cx + x]
            b = got_two[k * cx + x]
            row = (first + x) * ey
            above = jnp.where(side.even, a, b)
            below = jnp.where(side.even, b, a)
            out[rows_of(row, ov), :] = jnp.where(side.has_below, below, 0.0)
            out[rows_of(row + ov, cy), :] = part[x]
            out[rows_of(row + ov + cy, ov), :] = jnp.where(side.has_above, above, 0.0)
            return carry

        lax.fori_loop(0, cx, place, 0, unroll=24)

    edge = group_of(count, ov) * ey
    for ref, planes, first in ((field, count, 0), (coef, cx, edge)):

        def load(x, ref=ref):
            return ref[rows_of(x * ey, ey), :]

        last = first + group_of(planes, ov) * ey
        pack(load, planes, ey, ov, along.one(cz - ov, 0), one.at[first:last])
        pack(load, planes, ey, ov, along.two(cz - ov, 0), two.at[first:last])


def extended(field, got_one, got_two, x, count, ey, ov, along):
    halo = unpack(got_one, x, count, ey, ov, along.one(0, LANES - ov), along.one_valid)
    halo = halo + unpack(got_two, x, count, ey, ov, along.two(0, LANES - ov), along.two_valid)
    return jnp.concatenate([field[rows_of(x * ey, ey), :], halo], axis=1)


def turn(value):
    group = LANES // 8
    row = lax.broadcasted_iota(jnp.int32, (8, LANES), 0)
    column = lane_of((8, LANES)) // group
    for bit in (4, 2, 1):
        up = pltpu.roll(pltpu.roll(value, 8 - bit, 0), bit * group, 1)
        down = pltpu.roll(pltpu.roll(value, bit, 0), LANES - bit * group, 1)
        moved = jnp.where((row & bit) == 0, up, down)
        value = jnp.where((row & bit) == (column & bit), value, moved)
    return value


def solve(source, store, tables, state, count, back, ey, cx):
    z_on, z_back, y_on, y_back, x_on, x_back, recip = tables
    s0, s1 = state
    modes = recip.shape[1]
    group = LANES // 8
    lane = lane_of((ey, LANES))
    octs = ey // 8
    nothing = jnp.zeros((ey, LANES), F32)

    def times_y(table, core, sides):
        planes = [core[j * ey : (j + 1) * ey] for j in range(cx)] + sides
        planes += [nothing] * (-len(planes) % 4)
        done = []
        for j in range(0, len(planes), 4):
            quad = jnp.concatenate([jnp.concatenate(planes[j + i : j + i + 2], axis=0) for i in (0, 2)], axis=1)
            quad = dot(table[...], stack_rows(quad))
            done += [quad[i * ey : (i + 1) * ey, k * LANES : (k + 1) * LANES] for k in range(2) for i in range(2)]
        return done[:cx], done[cx : cx + len(sides)]

    def on(part, carry):
        rows = []
        for j in range(cx):
            value = source(part * cx + j)
            high, low = split(value[:, :LANES])
            near = value[:, LANES:].astype(BF16).astype(F32)
            halo = near + pltpu.roll(value[:, LANES:] - near, group, 1) + pltpu.roll(near, 2 * group, 1)
            rows.append((high, low, high, halo.astype(BF16)))
        value = dot(jnp.concatenate([jnp.concatenate(piece, axis=0) for piece in zip(*rows)], axis=1), z_on[...])
        sides = []
        for k in range(cx // 8):
            side = nothing
            for j in range(8):
                turned = pltpu.roll(value[(8 * k + j) * ey : (8 * k + j + 1) * ey, LANES:], j * group, 1)
                side = jnp.where(lane // group == j, turned, side)
            sides.append(side)
        core, sides = times_y(y_on, value[:, :LANES], sides)
        for j in range(cx):
            s0[rows_of((part * cx + j) * ey, ey), :] = core[j]
        for k in range(cx // 8):
            for q in range(octs):
                s1[rows_of(q * count + part * cx + k * 8, 8), :] = turn(sides[k][q * 8 : (q + 1) * 8])
        return carry

    lax.fori_loop(0, count // cx, on, 0, unroll=2)

    def times_x(value, factor):
        value = dot(x_on[...], stack_rows(value))
        value = jnp.concatenate([value[i * modes : (i + 1) * modes] * factor for i in range(value.shape[0] // modes)], axis=0)
        return dot(x_back[:back], stack_rows(value))

    def middle(h, carry):
        q = 2 * h
        value = [s0[pl.ds(q + i, count, stride=ey), :] for i in range(2)]
        value = times_x(jnp.concatenate(value, axis=1), jnp.concatenate([recip[q], recip[q + 1]], axis=1))
        for i in range(2):
            s0[pl.ds(q + i, back, stride=ey), :] = value[:, i * LANES : (i + 1) * LANES]
        return carry

    for q in range(octs):
        value = times_x(s1[q * count : (q + 1) * count, :], recip[ey + q])
        s1[q * count : q * count + back, :] = value
    lax.fori_loop(0, ey // 2, middle, 0, unroll=20)

    def off(part, carry):
        sides = []
        for k in range(cx // 8):
            sides.append(jnp.concatenate([turn(s1[rows_of(q * count + part * cx + k * 8, 8), :]) for q in range(octs)], axis=0))
        core, sides = times_y(y_back, s0[rows_of(part * cx * ey, cx * ey), :], sides)
        rows = []
        for k in range(cx // 8):
            near = sides[k].astype(BF16).astype(F32)
            far = sides[k] - near
            for j in range(8):
                high, low = split(core[8 * k + j])
                halo = [pltpu.roll(piece, (i - j) * group % LANES, 1) for i, piece in enumerate((near, far, near))]
                halo = jnp.where(lane < group, halo[0], jnp.where(lane < 2 * group, halo[1], halo[2]))
                rows.append((high, low, high, halo.astype(BF16)))
        value = dot(jnp.concatenate([jnp.concatenate(piece, axis=0) for piece in zip(*rows)], axis=1), z_back[...])
        for j in range(cx):
            store(part * cx + j, value[j * ey : (j + 1) * ey])
        return carry

    lax.fori_loop(0, back // cx, off, 0, unroll=2 if back > cx else 1)


def merged(core, halo, low):
    lane = lane_of(core.shape)
    return jnp.where((lane < LANES // 2) == low, core, halo)


def first_solve(info, field, got_one, got_two, z_on, z_back, y_on, y_back, x_on, x_back, recip, u, block, rest, one, two, s0, s1, *, nz, ov, ey, cx, cz):
    along = Side(info[2], nz)
    count = field.shape[0] // ey
    w = 2 * ov + 1
    edge, half = group_of(count, ov) * ey, rest.shape[0] // 2
    rest[:half] = got_one[edge:]
    rest[half:] = got_two[edge:]

    def source(x):
        value = extended(field, got_one, got_two, x, count, ey, ov, along)
        block[rows_of(x * ey, ey), :] = value
        return value

    def store(x, value):
        u[rows_of(x * ey, ey), :] = value

    solve(source, store, (z_on, z_back, y_on, y_back, x_on, x_back, recip), (s0, s1), count, count, ey, cx)

    for out, low in ((one, ~along.even), (two, along.even)):

        def load(x, low=low):
            rows = rows_of(x * ey, ey)
            return merged(u[rows, :LANES], u[rows, LANES:], low)

        pack(load, count, ey, w, jnp.where(low, LANES - ov, cz - ov - 1), out)


def sum_z(info, u, got_one, got_two, core_out, rest_out, one, two, *, ny, nz, ov, ey, cz):
    side, along = Side(info[1], ny), Side(info[2], nz)
    count = u.shape[0] // ey
    w = 2 * ov + 1
    lane = lane_of((ey, LANES))
    inside = ((lane <= ov) & along.has_above) | ((lane >= LANES - ov - 1) & along.has_below)

    def add(x, carry):
        rows = rows_of(x * ey, ey)
        core, rest = u[rows, :LANES], u[rows, LANES:]
        for got, low, valid in ((got_one, ~along.even, along.one_valid), (got_two, along.even, along.two_valid)):
            part = unpack(got, x, count, ey, w, jnp.where(low, LANES - ov - 1, cz - ov), valid)
            mine = (lane < LANES // 2) == low
            core, rest = core + jnp.where(mine, part, 0.0), rest + jnp.where(mine, 0.0, part)
        core_out[rows, :] = core
        rest_out[rows, :] = jnp.where(inside, rest, 0.0)
        return carry

    lax.fori_loop(0, count, add, 0, unroll=16)
    tall, halo = 2 * ov, 2 * (ov + 1)
    wide = group_of(count, halo)
    for out, high in ((one, side.even), (two, ~side.even)):
        start = jnp.where(high, ey - tall, 0)
        odd = pl.ds(jnp.where(high, ey - tall - 1, tall), count, stride=ey)

        def main(x, carry, out=out, start=start):
            out[rows_of(x * tall, tall), :] = core_out[rows_of(x * ey + start, tall), :]
            return carry

        lax.fori_loop(0, count, main, 0, unroll=16)
        base = count * tall

        def load(x, start=start):
            return rest_out[rows_of(x * ey + start, tall), :]

        pack(load, count, tall, halo, LANES - ov - 1, out.at[base : base + wide * tall])
        base = base + wide * tall
        out[base : base + count, :] = core_out[odd, :]
        rows = rest_out[odd, :]
        each = odd_group(count, halo)
        near = lane_of((each, LANES))
        value = jnp.zeros((each, LANES), F32)
        for g in range(count // each):
            turned = pltpu.roll(rows[g * each : (g + 1) * each], (g * halo + ov + 1) % LANES, 1)
            value = jnp.where((near >= g * halo) & (near < (g + 1) * halo), turned, value)
        out[base + count :, :] = value


def coefficients(info, *refs, nz, ov, ey):
    parts, out = refs[:-1], refs[-1]
    along = Side(info[2], nz)
    half = len(parts) // 2
    cx = parts[0].shape[0] // ey
    for k in range(half):
        core, rest = parts[k], parts[half + k]
        edge = rest.shape[0] // 2

        def plane(x, carry, k=k, core=core, rest=rest, edge=edge):
            value = extended(core, rest.at[:edge], rest.at[edge:], x, cx, ey, ov, along)
            out[rows_of((k * cx + x) * ey, ey), :] = value + 5.0
            return carry

        lax.fori_loop(0, cx, plane, 0, unroll=12)


def second_solve(info, core_in, rest_in, got_one, got_two, block, coef, z_on, z_back, y_on, y_back, x_on, x_back, recip, u, first, one, two, s0, s1, core_v, rest_v, far, *, ny, nz, ov, ey, cx, cz):
    side, along = Side(info[1], ny), Side(info[2], nz)
    count = coef.shape[0] // ey
    tall, halo = 2 * ov, 2 * (ov + 1)
    each = group_of(count, halo)
    room = ey + 2 * ov
    cy = ey - 2 * ov
    main_rows = count * tall
    odd_rows = main_rows + each * tall

    def sides(a, b):
        a, b = jnp.where(side.one_valid, a, 0.0), jnp.where(side.two_valid, b, 0.0)
        return jnp.where(side.even, b, a), jnp.where(side.even, a, b)

    def gather(x, carry):
        rows, slab = rows_of(x * ey, ey), rows_of(x * tall, tall)
        for source, out, (a, b) in (
            (core_in, core_v, (got_one[slab, :], got_two[slab, :])),
            (
                rest_in,
                rest_v,
                [unpack(got.at[main_rows:odd_rows], x, count, tall, halo, LANES - ov - 1, True) for got in (got_one, got_two)],
            ),
        ):
            below, above = sides(a, b)
            value = source[rows, :]
            low, high = value[:tall] + below, value[ey - tall :] + above
            out[rows_of(x * room + ov, ov), :] = jnp.where(side.has_below, low[:ov], 0.0)
            out[rows_of(x * room + tall, ov), :] = low[ov:]
            out[rows_of(x * room + ov + tall, ey - 2 * tall), :] = value[tall : ey - tall]
            out[rows_of(x * room + ov + ey - tall, ov), :] = high[:ov]
            out[rows_of(x * room + ey, ov), :] = jnp.where(side.has_above, high[ov:], 0.0)
        return carry

    lax.fori_loop(0, count, gather, 0, unroll=16)
    single = odd_group(count, halo)
    near = lane_of((single, LANES))

    def odd(ref):
        value = ref[odd_rows + count :, :]
        rows = [pltpu.roll(value, (2 * LANES - g * halo - ov - 1) % LANES, 1) for g in range(count // single)]
        return jnp.concatenate([jnp.where((near <= ov) | (near >= LANES - ov - 1), row, 0.0) for row in rows], axis=0)

    for out, a, b in (
        (core_v, got_one[odd_rows : odd_rows + count, :], got_two[odd_rows : odd_rows + count, :]),
        (rest_v, odd(got_one), odd(got_two)),
    ):
        below, above = sides(a, b)
        out[pl.ds(ov - 1, count, stride=room), :] = below
        out[pl.ds(ov + ey, count, stride=room), :] = above

    lane = lane_of((ey, RING))
    y = lax.broadcasted_iota(jnp.int32, (ey, RING), 0)
    inside = (lane < cz) | ((lane < cz + ov) & along.has_above) | ((lane >= RING - ov) & along.has_below)
    inside = inside & ((y >= ov) | side.has_below) & ((y < ey - ov) | side.has_above)

    def plane(x):
        at = (info[0] * cx + x) % count
        before, after = jnp.where(at > 0, 1.0, 0.0), jnp.where(at < count - 1, 1.0, 0.0)
        spots = [(x + shift) % count * room + ov for shift in (0, count - 1, 1)]
        halves = []
        for ref in (core_v, rest_v):
            mid, left, right = [ref[rows_of(spot, ey), :] for spot in spots]
            mid_y, left_y, right_y = [ref[pl.ds(spot - 1, ey), :] + ref[pl.ds(spot + 1, ey), :] for spot in spots]
            across, corner = before * left + after * right, before * left_y + after * right_y
            faces = mid_y + across
            halves.append((mid, 0.5 * faces + 0.125 * corner, 0.5 * mid + 0.125 * faces + 0.0625 * corner))
        mid, flat, slope = [jnp.concatenate(pair, axis=1) for pair in zip(*halves)]
        rows = rows_of(x * ey, ey)
        value = block[rows, :] - coef[rows, :] * mid + flat + (pltpu.roll(slope, 1, 1) + pltpu.roll(slope, RING - 1, 1))
        return jnp.where(inside, value, 0.0)

    def store(x, value):
        rows = rows_of(x * ey, ey)
        u[rows, :] = value[:, :LANES]
        far[rows, :] = value[:, LANES:]

    solve(plane, store, (z_on, z_back, y_on, y_back, x_on, x_back, recip), (s0, s1), count, cx, ey, cx)

    def load(x):
        return far[rows_of(x * ey, ey), :]

    pack(load, cx, ey, ov, along.one(0, LANES - ov), one)
    pack(load, cx, ey, ov, along.two(0, LANES - ov), two)

    def keep(x, carry):
        first[rows_of(x * cy, cy), :] = core_v[rows_of(x * room + 2 * ov, cy), :]
        return carry

    lax.fori_loop(0, cx, keep, 0, unroll=24)


def last_sum_z(info, u, got_one, got_two, v, one, two, *, ny, nz, ov, ey, cx, cz):
    side, along = Side(info[1], ny), Side(info[2], nz)

    def add(x, carry):
        rows = rows_of(x * ey, ey)
        value = u[rows, :]
        value = value + unpack(got_one, x, cx, ey, ov, along.one(cz - ov, 0), along.one_valid)
        value = value + unpack(got_two, x, cx, ey, ov, along.two(cz - ov, 0), along.two_valid)
        v[rows, :] = value
        one[rows_of(x * ov, ov), :] = v[rows_of(x * ey + side.one(ey - ov, 0), ov), :]
        two[rows_of(x * ov, ov), :] = v[rows_of(x * ey + side.two(ey - ov, 0), ov), :]
        return carry

    lax.fori_loop(0, cx, add, 0, unroll=24)


def last_sum_y(info, v, got_one, got_two, first, out, *, ny, ov, ey, cx):
    side = Side(info[1], ny)
    cy = ey - 2 * ov

    def add(x, carry):
        a, b = got_one[rows_of(x * ov, ov), :], got_two[rows_of(x * ov, ov), :]
        above, below = jnp.where(side.even, a, b), jnp.where(side.even, b, a)
        above, below = jnp.where(side.has_above, above, 0.0), jnp.where(side.has_below, below, 0.0)
        value = v[rows_of(x * ey + ov, cy), :] + first[rows_of(x * cy, cy), :]
        out[x] = jnp.concatenate([value[:ov] + below, value[ov : cy - ov], value[cy - ov :] + above], axis=0)
        return carry

    lax.fori_loop(0, cx, add, 0, unroll=24)


def make_tables(info, eigen_x, rest, zt, out, z_on, z_back, *, ov, ez):
    def row(q, carry):
        out[q] = 1.0 / (eigen_x[...] + rest[pl.ds(q, 1), :])
        return carry

    lax.fori_loop(0, out.shape[0], row, 0, unroll=5)

    def fill(table, ref, halo):
        high = table.astype(BF16).astype(F32)
        low = table - high
        ref[:LANES] = high[:LANES].astype(BF16)
        ref[LANES : 2 * LANES] = high[:LANES].astype(BF16)
        ref[2 * LANES : 3 * LANES] = low[:LANES].astype(BF16)
        ref[3 * LANES :] = halo(high, low).astype(BF16)

    def ring(high, low):
        above, below = slice(LANES, LANES + ov), slice(RING - ov, RING)
        parts = [high[above], high[below], high[above], low[below], low[above], jnp.zeros((LANES - 6 * ov, RING), F32), high[below]]
        return jnp.concatenate(parts, axis=0)

    def plain(high, low):
        tail = slice(LANES, ez)
        parts = [high[tail], high[tail], low[tail], jnp.zeros((LANES - 3 * (ez - LANES), RING), F32)]
        return jnp.concatenate(parts, axis=0)

    table = zt[...]
    fill(table, z_on, ring)
    fill(table.T, z_back, plain)


def gather_x(block):
    count = lax.axis_size("gx")
    parts = [block]
    for shift in range(1, count):
        parts.append(lax.ppermute(block, "gx", [((i + shift) % count, i) for i in range(count)]))
    return parts


def columns(table):
    high = lax.reduce_precision(table, 8, 7)
    return jnp.concatenate([high, table - high, high], axis=1).astype(BF16)


def local(right_side, reaction, basis_x, basis_y, basis_z, eigen_x, eigen_y, eigen_z):
    cx, cy, cz = right_side.shape
    ex, ey, ez = basis_x.shape[0], basis_y.shape[0], basis_z.shape[0]
    ov = (ex - cx) // 2
    nx, ny, nz = lax.axis_size("gx"), lax.axis_size("gy"), lax.axis_size("gz")
    ix = lax.axis_index("gx")
    count = nx * cx
    w, tall, halo = 2 * ov + 1, 2 * ov, 2 * (ov + 1)
    at = dict(ov=ov, ey=ey, cz=cz)

    f_parts = gather_x(right_side)

    blocks = [jnp.pad(basis_x.T, ((0, 0), (i * cx, (nx - 1 - i) * cx)))[:, ov : ov + count] for i in range(nx)]
    table = jnp.concatenate(blocks, axis=0)
    table = lax.dynamic_slice_in_dim(jnp.concatenate([table, table], axis=1), ix * cx, count, axis=1)
    zero = jnp.zeros((ey, ey), F32)
    double = jnp.concatenate([jnp.concatenate([basis_y, zero], axis=1), jnp.concatenate([zero, basis_y], axis=1)], axis=0)
    zt = jnp.concatenate([basis_z[ov:], jnp.zeros((RING - ez, ez), F32), basis_z[:ov]], axis=0)
    zt = jnp.pad(zt, ((0, 0), (0, RING - ez)))
    rest = eigen_y[:, None] + eigen_z[None, :]
    rest = jnp.concatenate([rest[:, :LANES], rest[:, LANES:].reshape(-1, LANES)], axis=0)
    recip, z_on, z_back = call(
        functools.partial(make_tables, ov=ov, ez=ez), [(rest.shape[0], ex, LANES), (4 * LANES, RING, BF16), (4 * LANES, RING, BF16)],
        jnp.broadcast_to(eigen_x[:, None], (ex, LANES)), rest, zt,
    )
    tables = (z_on, z_back, columns(double.T), columns(double), columns(table), columns(table.T), recip)

    slabs = call(functools.partial(first_slabs, ny=ny, ov=ov), [(count + cx, ov, cz)] * 2, *f_parts, reaction)
    got = swap(*slabs, "gy")
    edge = group_of(cx, ov) * ey
    small = (group_of(count, ov) * ey + edge, LANES)
    f, c, *slabs = call(
        functools.partial(second_slabs, ny=ny, nz=nz, ov=ov), [(count * ey, cz), (cx * ey, cz), small, small], *f_parts, reaction, *got
    )
    got = swap(*slabs, "gz", around=True)
    c_parts = gather_x(c)
    state = [pltpu.VMEM((count * ey, LANES), F32), pltpu.VMEM((ey // 8 * count, LANES), F32)]
    small = (group_of(count, w) * ey, LANES)
    u, block, rest, *slabs = call(
        functools.partial(first_solve, nz=nz, cx=cx, **at), [(count * ey, RING)] * 2 + [(2 * edge, LANES), small, small], f, *got, *tables, scratch=state
    )
    got = swap(*slabs, "gz")
    c_parts += gather_x(rest)
    tall_rows = (count * tall + group_of(count, halo) * tall + count + odd_group(count, halo), LANES)
    core, rest, *slabs = call(functools.partial(sum_z, ny=ny, nz=nz, **at), [(count * ey, LANES)] * 2 + [tall_rows, tall_rows], u, *got)
    got = swap(*slabs, "gy")
    c = call(functools.partial(coefficients, nz=nz, ov=ov, ey=ey), [(count * ey, RING)], *c_parts, after=slabs[:1])[0]
    small = (group_of(cx, ov) * ey, LANES)
    state += [pltpu.VMEM((count * (ey + 2 * ov), LANES), F32)] * 2 + [pltpu.VMEM((cx * ey, LANES), F32)]
    u, first, *slabs = call(
        functools.partial(second_solve, ny=ny, nz=nz, cx=cx, **at),
        [(cx * ey, LANES), (cx * cy, LANES), small, small], core, rest, *got, block, c, *tables, scratch=state,
    )
    got = swap(*slabs, "gz", around=True)
    v, *slabs = call(functools.partial(last_sum_z, ny=ny, nz=nz, cx=cx, **at), [(cx * ey, LANES)] + [(cx * ov, LANES)] * 2, u, *got)
    got = swap(*slabs, "gy")
    return call(functools.partial(last_sum_y, ny=ny, ov=ov, ey=ey, cx=cx), [(cx, cy, cz)], v, *got, first)[0]


def solution(mesh):
    return jax.shard_map(
        local,
        mesh=mesh,
        in_specs=(P("gx", "gy", "gz"), P("gx", "gy", "gz"), P(), P(), P(), P(), P(), P()),
        out_specs=P("gx", "gy", "gz"),
        check_vma=False,
    )
```
